128 devices in a mesh: row: 4 (over z_lo, core), col: 32 (over z_hi, y, x).
Axes of the slice: x: 4, y: 4, z: 4 (z_hi: 2, z_lo: 2; z = z_hi * 2 + z_lo), core: 2. Of those that a mesh axis runs over, the one named last changes fastest.
Arguments:
- source_terms: float32 [256, 2048, 256], P('row', 'col'), may hold values from -6 to 6
- initial_values: float32 [256, 2048, 256], P('row', 'col'), may hold values from -6 to 6
- absorption: float32 [256, 2048, 256], P('row', 'col'), may hold values from 0.1 to 0.9
Outputs:
- improved: float32 [256, 2048, 256], P('row', 'col')
- remaining: float32 [256, 2048, 256], P('row', 'col')
The draws below stay inside these ranges and needn't reach their ends.
All inputs are finite; a program needn't handle non-finite values.
Results may differ from the reference program's by a relative error of at most 0.000043.
Values sent between devices are 32-bit elements; how exact they have to be, the bound alone decides.
A program may use at most 128 MiB of HBM per device.

```python
import jax
import jax.numpy as jnp
from jax import lax

LAYERS = 256
RATIO = 4
BEFORE = 3
AFTER = 3
INNER = 9
GRID_Y = 256
GRID_X = 2048


def shard_levels(key, dims, split, smallest, top_value):
    def one(axis_at, shards_of):
        steps = jax.random.uniform(jax.random.fold_in(jax.random.fold_in(key, 6), axis_at), (shards_of,), jnp.float32, smallest / len(split), top_value / len(split))
        return jnp.repeat(jnp.exp(steps), dims[axis_at] // shards_of).reshape((-1,) + (1,) * (len(dims) - axis_at - 1))

    factor_of = one(*split[0])
    for cut in split[1:]:
        factor_of = factor_of * one(*cut)
    return factor_of


def normal_values(own_key, dims, spread, limit, split=(), held_as=jnp.bfloat16):
    values = jax.random.normal(own_key, dims, jnp.float32) * spread
    if len(split) > 0:
        values = shard_levels(own_key, dims, split, -0.22, 0.18) * values
    return jnp.clip(values, min=-limit, max=limit).astype(held_as)


def setup_inputs(seed: int = 0) -> dict:
    arg_keys = jax.random.split(jax.random.key(seed), 4)
    return {
        "source_terms": normal_values(arg_keys[0], (GRID_Y, GRID_X, LAYERS), 1.0, 6.0, ((0, 4), (1, 32)), jnp.float32),
        "initial_values": normal_values(arg_keys[1], (GRID_Y, GRID_X, LAYERS), 1.0, 6.0, ((0, 4), (1, 32)), jnp.float32),
        "absorption": jnp.clip(0.1 + 0.79999997 * jax.random.uniform(arg_keys[2], (GRID_Y, GRID_X, LAYERS), jnp.float32) ** shard_levels(arg_keys[2], (GRID_Y, GRID_X, LAYERS), ((0, 4), (1, 32)), -0.2, 0.2), 0.1, 0.9),
    }


def cross_sum(padded):
    inner_y, inner_x = padded.shape[0] - 2, padded.shape[1] - 2
    middle_rows = lax.slice_in_dim(padded, 1, 1 + inner_y, axis=0)
    middle_columns = lax.slice_in_dim(padded, 1, 1 + inner_x, axis=1)
    return (lax.slice_in_dim(middle_columns, 0, inner_y, axis=0) + lax.slice_in_dim(middle_columns, 2, 2 + inner_y, axis=0)
            + lax.slice_in_dim(middle_rows, 0, inner_x, axis=1) + lax.slice_in_dim(middle_rows, 2, 2 + inner_x, axis=1))


def smooth_step(padded, values, load, mass_here):
    return values + 0.8 * (load + cross_sum(padded) - (4.0 + mass_here) * values) / (4.0 + mass_here)


def block_means(values):
    cut = values.reshape(values.shape[0] // RATIO, RATIO, values.shape[1] // RATIO, RATIO, values.shape[2])
    return jnp.mean(cut, axis=(1, 3))


def spread_blocks(values):
    return jnp.repeat(jnp.repeat(values, RATIO, axis=0), RATIO, axis=1)


def reference(source_terms, initial_values, absorption):
    values = initial_values
    for sweep in range(BEFORE):
        values = smooth_step(jnp.pad(values, ((1, 1), (1, 1), (0, 0)), mode="wrap"), values, source_terms, absorption)
    defect = source_terms + cross_sum(jnp.pad(values, ((1, 1), (1, 1), (0, 0)), mode="wrap")) - (4.0 + absorption) * values
    coarse_load, coarse_mass = block_means(defect) * RATIO, block_means(absorption) * RATIO
    coarse_values = jnp.zeros_like(coarse_load)
    for sweep in range(INNER):
        coarse_values = smooth_step(jnp.pad(coarse_values, ((1, 1), (1, 1), (0, 0)), mode="wrap"), coarse_values, coarse_load, coarse_mass)
    values = values + spread_blocks(coarse_values)
    for sweep in range(AFTER):
        values = smooth_step(jnp.pad(values, ((1, 1), (1, 1), (0, 0)), mode="wrap"), values, source_terms, absorption)
    improved = values
    remaining = source_terms + cross_sum(jnp.pad(improved, ((1, 1), (1, 1), (0, 0)), mode="wrap")) - (4.0 + absorption) * improved
    return improved, remaining
```

```python
import functools

import jax
import jax.numpy as jnp
from jax import lax
from jax.experimental import pallas as pl
from jax.experimental.pallas import tpu as pltpu
from jax.sharding import PartitionSpec as P

RATIO = 4
INNER = 9
LANES = 128
ROW_PAD = 4
COL_PAD = 8
DEEP = INNER
COARSE_PAD = 16
MESH = pl.DeviceIdType.MESH


def edge_rects(rows, cols, near, far):
    (y0, ny), (x0, nx) = rows, cols
    wide = far - near
    return [
        (0, 1, (y0, ny, x0 + nx - far, wide), (y0, ny, x0 - far, wide)),
        (0, -1, (y0, ny, x0 + near, wide), (y0, ny, x0 + nx + near, wide)),
        (1, 0, (y0 + ny - far, wide, x0, nx), (y0 - far, wide, x0, nx)),
        (-1, 0, (y0 + near, wide, x0, nx), (y0 + ny + near, wide, x0, nx)),
    ]


def corner_rects(rows, cols, near_y, far_y, far_x):
    (y0, ny), (x0, nx) = rows, cols
    wide = far_y - near_y
    found = []
    for dy in (1, -1):
        if dy == 1:
            from_y, to_y = y0 + ny - far_y, y0 - far_y
        else:
            from_y, to_y = y0 + near_y, y0 + ny + near_y
        for dx in (1, -1):
            if dx == 1:
                from_x, to_x = x0 + nx - far_x, x0 - far_x
            else:
                from_x, to_x = x0, x0 + nx
            found.append((dy, dx, (from_y, wide, from_x, far_x), (to_y, wide, to_x, far_x)))
    return found


def plan(ny, nx):
    rows, cols = (ROW_PAD, ny), (COL_PAD, nx)
    crows, ccols = (DEEP, ny // RATIO), (COARSE_PAD, nx // RATIO)
    coarse = edge_rects(crows, ccols, 0, DEEP)
    for step in range(3):
        coarse = coarse + corner_rects(crows, ccols, 3 * step, 3 * step + 3, DEEP - 3 * step)
    exchanges = {
        "u0": edge_rects(rows, cols, 0, 1),
        "f": edge_rects(rows, cols, 0, 2) + corner_rects(rows, cols, 0, 2, 2),
        "r": edge_rects(rows, cols, 0, 2) + corner_rects(rows, cols, 0, 2, 2),
        "u1": edge_rects(rows, cols, 0, 3) + corner_rects(rows, cols, 0, 2, 2),
        "cr": coarse,
        "f3": edge_rects(rows, cols, 2, 3),
        "r3": edge_rects(rows, cols, 2, 3),
        "cl": coarse,
        "u3": edge_rects(rows, cols, 0, 4) + corner_rects(rows, cols, 0, 3, 3),
    }
    at, first = 0, {}
    for name, rects in exchanges.items():
        first[name] = at
        at += len(rects)
    return exchanges, first, at


def kernel(sizes, f_hbm, u_hbm, a_hbm, improved_hbm, remaining_hbm,
           ua, ub, uc, ud, f, r, d, sums, spread, cl, cr, ca, cb,
           load_sem, store_sem, send_sem, recv_sem):
    ny, nx, halves, n_row, n_col = sizes
    cy, cx = ny // RATIO, nx // RATIO
    exchanges, first, _ = plan(ny, nx)
    me_row, me_col = lax.axis_index("row"), lax.axis_index("col")

    def neighbour(dy, dx):
        return (lax.rem(me_row + dy + n_row, n_row), lax.rem(me_col + dx + n_col, n_col))

    def box(ref, where):
        y, h, x, w = where
        return ref.at[pl.ds(y, h), :, pl.ds(x, w), :]

    def copies(name, source, landing):
        made = []
        for k, (dy, dx, src, dst) in enumerate(exchanges[name]):
            made.append(pltpu.make_async_remote_copy(
                src_ref=box(source, src), dst_ref=box(landing, dst),
                send_sem=send_sem.at[first[name] + k], recv_sem=recv_sem.at[first[name] + k],
                device_id=neighbour(dy, dx), device_id_type=MESH))
        return made

    sent = []

    def send(name, source, landing):
        made = copies(name, source, landing)
        for copy in made:
            copy.start()
        sent.append((name, made))
        return made

    def arrived(made):
        for copy in made:
            copy.wait_recv()

    def loads(k, hbm, ref, y0, x0):
        made = []
        for h in range(halves):
            made.append(pltpu.make_async_copy(
                hbm.at[:, :, pl.ds(h * LANES, LANES)],
                ref.at[pl.ds(y0, ny), h, pl.ds(x0, nx), :],
                load_sem.at[k * halves + h]))
        for copy in made:
            copy.start()
        return made

    a_loads = loads(0, a_hbm, d, 0, 0)
    u_loads = loads(1, u_hbm, ua, ROW_PAD, COL_PAD)
    f_loads = loads(2, f_hbm, f, ROW_PAD, COL_PAD)

    barrier = pltpu.get_barrier_semaphore()
    around = [(dy, dx) for dy in (-1, 0, 1) for dx in (-1, 0, 1) if (dy, dx) != (0, 0)]
    for dy, dx in around:
        pl.semaphore_signal(barrier, inc=1, device_id=neighbour(dy, dx), device_id_type=MESH)

    own = [COL_PAD + 8 * k for k in range(nx // 8)]

    def windows(x0, n, reach):
        low, high = x0 - reach, x0 + n + reach
        return [min(x, high - 8) for x in range(low, high, 8)]

    def at(ref, y, h, x):
        return ref[y, h, pl.ds(x, 8), :]

    def coarse_sums(ref, done):
        def body(y, carry):
            for h in range(halves):
                for g in range(cx // 8):
                    parts = [sums[y, h, pl.ds(32 * g + k, 8, stride=4), :] for k in range(4)]
                    total = ((parts[0] + parts[1]) + (parts[2] + parts[3])) * 0.25
                    done(y, h, g, total)
            return carry
        lax.fori_loop(0, cy, body, 0)

    for copy in a_loads:
        copy.wait()

    def prepare(y, carry):
        for h in range(halves):
            for k in range(nx // 8):
                total = None
                for j in range(RATIO):
                    a = d[RATIO * y + j, h, pl.ds(8 * k, 8), :]
                    here = 4.0 + a
                    d[RATIO * y + j, h, pl.ds(8 * k, 8), :] = here
                    r[ROW_PAD + RATIO * y + j, h, pl.ds(COL_PAD + 8 * k, 8), :] = 0.8 / here
                    total = a if total is None else total + a
                sums[y, h, pl.ds(8 * k, 8), :] = total
        return carry
    lax.fori_loop(0, cy, prepare, 0)

    def keep_mass(y, h, g, total):
        cr[DEEP + y, h, pl.ds(COARSE_PAD + 8 * g, 8), :] = 0.8 / (4.0 + total)
    coarse_sums(sums, keep_mass)

    pl.semaphore_wait(barrier, len(around))
    for copy in u_loads:
        copy.wait()
    u0 = send("u0", ua, ua)
    for copy in f_loads:
        copy.wait()
    f2 = send("f", f, f)
    r2 = send("r", r, r)

    def sweep(src, dst, reach, starts, load, rate, top, count, step=2):
        def body(i, carry):
            y = top - reach + step * i
            for h in range(halves):
                for x in starts:
                    column = [at(src, y + j, h, x) for j in range(-1, step + 1)]
                    for j in range(step):
                        total = (column[j] + column[j + 2]) + (at(src, y + j, h, x - 1) + at(src, y + j, h, x + 1))
                        new = 0.2 * column[j + 1] + at(rate, y + j, h, x) * (at(load, y + j, h, x) + total)
                        dst[y + j, h, pl.ds(x, 8), :] = new
            return carry
        lax.fori_loop(0, (count + 2 * reach) // step, body, 0)

    def left_over(src, y, h, x):
        column = [at(src, y + j, h, x) for j in range(-1, RATIO + 1)]
        found = []
        for j in range(RATIO):
            total = (column[j] + column[j + 2]) + (at(src, y + j, h, x - 1) + at(src, y + j, h, x + 1))
            here = d[y + j - ROW_PAD, h, pl.ds(x - COL_PAD, 8), :]
            found.append((at(f, y + j, h, x) + total) - here * column[j + 1])
        return found

    arrived(u0)
    sweep(ua, ub, 0, own, f, r, ROW_PAD, ny)
    u1 = send("u1", ub, ub)
    coarse_mass = send("cr", cr, cr)
    f3 = send("f3", f, f)
    r3 = send("r3", r, r)
    for copy in u0:
        copy.wait_send()
    arrived(f2)
    arrived(r2)
    arrived(u1)
    sweep(ub, ua, 2, windows(COL_PAD, nx, 2), f, r, ROW_PAD, ny)
    sweep(ua, uc, 1, windows(COL_PAD, nx, 1), f, r, ROW_PAD, ny)

    def defect(y, carry):
        for h in range(halves):
            for k, x in enumerate(own):
                a, b, c, e = left_over(uc, ROW_PAD + RATIO * y, h, x)
                sums[y, h, pl.ds(8 * k, 8), :] = (a + b) + (c + e)
        return carry
    lax.fori_loop(0, cy, defect, 0)

    def keep_load(y, h, g, total):
        cl[DEEP + y, h, pl.ds(COARSE_PAD + 8 * g, 8), :] = total
    coarse_sums(sums, keep_load)
    coarse_load = send("cl", cl, cl)
    u3 = send("u3", uc, ud)

    arrived(coarse_mass)
    arrived(coarse_load)

    def first_coarse(y, carry):
        for h in range(halves):
            for x in windows(COARSE_PAD, cx, DEEP):
                ca[y, h, pl.ds(x, 8), :] = at(cr, y, h, x) * at(cl, y, h, x)
        return carry
    lax.fori_loop(0, cy + 2 * DEEP, first_coarse, 0)

    now, later = ca, cb
    for reach in range(DEEP - 1, 0, -1):
        sweep(now, later, reach, windows(COARSE_PAD, cx, reach), cl, cr, DEEP, cy)
        now, later = later, now

    def spread_row(y, carry):
        for h in range(halves):
            for w in range((cx + 2 + 7) // 8):
                c = at(now, DEEP - 1 + y, h, COARSE_PAD - 1 + 8 * w)
                for k in range(RATIO):
                    spread[y, h, pl.ds(32 * w + k, 8, stride=4), :] = c
        return carry
    lax.fori_loop(0, cy + 2, spread_row, 0)

    arrived(f3)
    arrived(r3)
    arrived(u3)

    def correct(y, carry):
        for h in range(halves):
            for x in own:
                add = spread[y, h, pl.ds(x - COL_PAD + 4, 8), :]
                for j in range(RATIO):
                    ua[RATIO * y + j, h, pl.ds(x, 8), :] = at(uc, RATIO * y + j, h, x) + add
            for x in (COL_PAD - 4, COL_PAD + nx):
                add = spread[y, h, pl.ds(x - COL_PAD + 4, 4), :]
                for j in range(RATIO):
                    ua[RATIO * y + j, h, pl.ds(x, 4), :] = ud[RATIO * y + j, h, pl.ds(x, 4), :] + add
        return carry
    lax.fori_loop(1, cy + 1, correct, 0)

    for y in (0, cy + 1):
        def correct_edge(j, carry):
            for h in range(halves):
                for x in windows(COL_PAD, nx, 4):
                    add = spread[y, h, pl.ds(x - COL_PAD + 4, 8), :]
                    ua[RATIO * y + j, h, pl.ds(x, 8), :] = at(ud, RATIO * y + j, h, x) + add
            return carry
        lax.fori_loop(0, RATIO, correct_edge, 0)

    for copy in u1:
        copy.wait_send()
    sweep(ua, ub, 3, windows(COL_PAD, nx, 3), f, r, ROW_PAD, ny)
    sweep(ub, ua, 2, windows(COL_PAD, nx, 2), f, r, ROW_PAD, ny)
    sweep(ua, ub, 1, windows(COL_PAD, nx, 1), f, r, ROW_PAD, ny)

    def stores(k, ref, hbm, y, rows):
        made = []
        for h in range(halves):
            made.append(pltpu.make_async_copy(
                ref.at[pl.ds(ROW_PAD + y, rows), h, pl.ds(COL_PAD, nx), :],
                hbm.at[pl.ds(y, rows), :, pl.ds(h * LANES, LANES)],
                store_sem.at[k * halves + h]))
        for copy in made:
            copy.start()
        return made

    going = stores(0, ub, improved_hbm, 0, ny)
    parts = 4
    for part in range(parts):
        def remain(y, carry):
            for h in range(halves):
                for x in own:
                    for j, found in enumerate(left_over(ub, ROW_PAD + RATIO * y, h, x)):
                        ua[ROW_PAD + RATIO * y + j, h, pl.ds(x, 8), :] = found
            return carry
        lax.fori_loop(part * cy // parts, (part + 1) * cy // parts, remain, 0)
        going += stores(1 + part, ua, remaining_hbm, part * ny // parts, ny // parts)

    for name, made in sent:
        if name not in ("u0", "u1"):
            for copy in made:
                copy.wait_send()
    for copy in going:
        copy.wait()


def local(n_row, n_col, source_terms, initial_values, absorption):
    ny, nx, layers = source_terms.shape
    halves = layers // LANES
    sizes = (ny, nx, halves, n_row, n_col)
    _, _, count = plan(ny, nx)
    fine = pltpu.VMEM((ny + 2 * ROW_PAD, halves, nx + 2 * COL_PAD, LANES), jnp.float32)
    block = pltpu.VMEM((ny, halves, nx, LANES), jnp.float32)
    cy, cx = ny // RATIO, nx // RATIO
    coarse = pltpu.VMEM((cy + 2 * DEEP, halves, cx + 2 * COARSE_PAD, LANES), jnp.float32)
    anywhere = pl.BlockSpec(memory_space=pltpu.HBM)
    shape = jax.ShapeDtypeStruct(source_terms.shape, jnp.float32)
    return pl.pallas_call(
        functools.partial(kernel, sizes),
        out_shape=(shape, shape),
        in_specs=[anywhere] * 3,
        out_specs=(anywhere, anywhere),
        scratch_shapes=[
            fine, fine, fine, fine, fine, fine, block,
            pltpu.VMEM((cy, halves, nx, LANES), jnp.float32),
            pltpu.VMEM((cy + 2, halves, (cx + 8) * RATIO, LANES), jnp.float32),
            coarse, coarse, coarse, coarse,
            pltpu.SemaphoreType.DMA((3 * halves,)),
            pltpu.SemaphoreType.DMA((5 * halves,)),
            pltpu.SemaphoreType.DMA((count,)),
            pltpu.SemaphoreType.DMA((count,)),
        ],
        compiler_params=pltpu.CompilerParams(
            collective_id=0, has_side_effects=True, vmem_limit_bytes=66_000_000
        ),
        name="two_grids",
    )(source_terms, initial_values, absorption)


def solution(mesh):
    n_row, n_col = mesh.shape["row"], mesh.shape["col"]
    spec = P("row", "col", None)
    return jax.shard_map(
        functools.partial(local, n_row, n_col),
        mesh=mesh, in_specs=(spec, spec, spec), out_specs=(spec, spec), check_vma=False,
    )
```

```python
import functools

import jax
import jax.numpy as jnp
from jax import lax
from jax.experimental import pallas as pl
from jax.experimental.pallas import tpu as pltpu
from jax.sharding import PartitionSpec as P

RATIO = 4
INNER = 9
LANES = 128
ROW_PAD = 4
COL_PAD = 8
FIRST = 5
DEEP = INNER - FIRST + 1
COARSE_PAD = 8
MESH = pl.DeviceIdType.MESH


def edge_rects(rows, cols, near, far):
    (y0, ny), (x0, nx) = rows, cols
    wide = far - near
    return [
        (0, 1, (y0, ny, x0 + nx - far, wide), (y0, ny, x0 - far, wide)),
        (0, -1, (y0, ny, x0 + near, wide), (y0, ny, x0 + nx + near, wide)),
        (1, 0, (y0 + ny - far, wide, x0, nx), (y0 - far, wide, x0, nx)),
        (-1, 0, (y0 + near, wide, x0, nx), (y0 + ny + near, wide, x0, nx)),
    ]


def corner_rects(rows, cols, near_y, far_y, far_x):
    (y0, ny), (x0, nx) = rows, cols
    wide = far_y - near_y
    found = []
    for dy in (1, -1):
        if dy == 1:
            from_y, to_y = y0 + ny - far_y, y0 - far_y
        else:
            from_y, to_y = y0 + near_y, y0 + ny + near_y
        for dx in (1, -1):
            if dx == 1:
                from_x, to_x = x0 + nx - far_x, x0 - far_x
            else:
                from_x, to_x = x0, x0 + nx
            found.append((dy, dx, (from_y, wide, from_x, far_x), (to_y, wide, to_x, far_x)))
    return found


def plan(ny, nx):
    rows, cols = (ROW_PAD, ny), (COL_PAD, nx)
    crows, ccols = (DEEP, ny // RATIO), (COARSE_PAD, nx // RATIO)
    coarse = edge_rects(crows, ccols, 0, DEEP - 1)
    coarse = coarse + corner_rects(crows, ccols, 0, 2, 4) + corner_rects(crows, ccols, 2, 4, 2)
    values = edge_rects(crows, ccols, 0, DEEP)
    values = values + corner_rects(crows, ccols, 0, 3, 5) + corner_rects(crows, ccols, 3, 5, 2)
    exchanges = {
        "u0": edge_rects(rows, cols, 0, 1),
        "f": edge_rects(rows, cols, 0, 2) + corner_rects(rows, cols, 0, 2, 2),
        "r": edge_rects(rows, cols, 0, 2) + corner_rects(rows, cols, 0, 2, 2),
        "u1": edge_rects(rows, cols, 0, 3) + corner_rects(rows, cols, 0, 2, 2),
        "cr": coarse,
        "f3": edge_rects(rows, cols, 2, 3),
        "r3": edge_rects(rows, cols, 2, 3),
        "cl": coarse,
        "u3": edge_rects(rows, cols, 1, 4) + corner_rects(rows, cols, 0, 3, 3),
        "cv": values,
    }
    at, first = 0, {}
    for name, rects in exchanges.items():
        first[name] = at
        at += len(rects)
    return exchanges, first, at


def left_over(u, f, d, y, h, x):
    column = [u[y + j, h, pl.ds(x, 8), :] for j in range(-1, RATIO + 1)]
    found = []
    for j in range(RATIO):
        beside = u[y + j, h, pl.ds(x - 1, 8), :] + u[y + j, h, pl.ds(x + 1, 8), :]
        total = f[y + j, h, pl.ds(x, 8), :] + ((column[j] + column[j + 2]) + beside)
        found.append(total - d[y + j - ROW_PAD, h, pl.ds(x - COL_PAD, 8), :] * column[j + 1])
    return found


def finish(sizes, u, f, d, improved_hbm, remaining_hbm, left, store_sem):
    ny, nx, halves = sizes
    cy = ny // RATIO

    def stores(k, ref, hbm, y0, x0, y, rows):
        made = []
        for h in range(halves):
            made.append(pltpu.make_async_copy(
                ref.at[pl.ds(y0 + y, rows), h, pl.ds(x0, nx), :],
                hbm.at[pl.ds(y, rows), :, pl.ds(h * LANES, LANES)],
                store_sem.at[k * halves + h]))
        for copy in made:
            copy.start()
        return made

    going = stores(0, u, improved_hbm, ROW_PAD, COL_PAD, 0, ny)
    parts = 4
    for part in range(parts):
        def remain(y, carry):
            for h in range(halves):
                for k in range(nx // 8):
                    for j, found in enumerate(left_over(u, f, d, ROW_PAD + RATIO * y, h, COL_PAD + 8 * k)):
                        left[RATIO * y + j, h, pl.ds(8 * k, 8), :] = found
            return carry
        lax.fori_loop(part * cy // parts, (part + 1) * cy // parts, remain, 0)
        going += stores(1 + part, left, remaining_hbm, 0, 0, part * ny // parts, ny // parts)
    for copy in going:
        copy.wait()


def kernel(sizes, f_hbm, u_hbm, a_hbm, ub, f, d,
           ua, uc, ud, r, sums, spread, cl, cr, ca, cb, cc,
           load_sem, send_sem, recv_sem):
    ny, nx, halves, n_row, n_col = sizes
    cy, cx = ny // RATIO, nx // RATIO
    exchanges, first, _ = plan(ny, nx)
    me_row, me_col = lax.axis_index("row"), lax.axis_index("col")

    def neighbour(dy, dx):
        return (lax.rem(me_row + dy + n_row, n_row), lax.rem(me_col + dx + n_col, n_col))

    def box(ref, where):
        y, h, x, w = where
        return ref.at[pl.ds(y, h), :, pl.ds(x, w), :]

    def copies(name, source, landing):
        made = []
        for k, (dy, dx, src, dst) in enumerate(exchanges[name]):
            made.append(pltpu.make_async_remote_copy(
                src_ref=box(source, src), dst_ref=box(landing, dst),
                send_sem=send_sem.at[first[name] + k], recv_sem=recv_sem.at[first[name] + k],
                device_id=neighbour(dy, dx), device_id_type=MESH))
        return made

    sent = []

    def send(name, source, landing):
        made = copies(name, source, landing)
        for copy in made:
            copy.start()
        sent.append((name, made))
        return made

    def arrived(made):
        for copy in made:
            copy.wait_recv()

    def loads(k, hbm, ref, y0, x0):
        made = []
        for h in range(halves):
            made.append(pltpu.make_async_copy(
                hbm.at[:, :, pl.ds(h * LANES, LANES)],
                ref.at[pl.ds(y0, ny), h, pl.ds(x0, nx), :],
                load_sem.at[k * halves + h]))
        for copy in made:
            copy.start()
        return made

    a_loads = loads(0, a_hbm, d, 0, 0)
    u_loads = loads(1, u_hbm, ua, ROW_PAD, COL_PAD)
    f_loads = loads(2, f_hbm, f, ROW_PAD, COL_PAD)

    barrier = pltpu.get_barrier_semaphore()
    around = [(dy, dx) for dy in (-1, 0, 1) for dx in (-1, 0, 1) if (dy, dx) != (0, 0)]
    for dy, dx in around:
        pl.semaphore_signal(barrier, inc=1, device_id=neighbour(dy, dx), device_id_type=MESH)

    own = [COL_PAD + 8 * k for k in range(nx // 8)]

    def windows(x0, n, reach):
        low, high = x0 - reach, x0 + n + reach
        return [min(x, high - 8) for x in range(low, high, 8)]

    def at(ref, y, h, x):
        return ref[y, h, pl.ds(x, 8), :]

    def coarse_sums(ref, done):
        def body(y, carry):
            for h in range(halves):
                for g in range(cx // 8):
                    parts = [sums[y, h, pl.ds(32 * g + k, 8, stride=4), :] for k in range(4)]
                    total = ((parts[0] + parts[1]) + (parts[2] + parts[3])) * 0.25
                    done(y, h, g, total)
            return carry
        lax.fori_loop(0, cy, body, 0)

    for copy in a_loads:
        copy.wait()

    def prepare(y, carry):
        for h in range(halves):
            for k in range(nx // 8):
                total = None
                for j in range(RATIO):
                    a = d[RATIO * y + j, h, pl.ds(8 * k, 8), :]
                    here = 4.0 + a
                    d[RATIO * y + j, h, pl.ds(8 * k, 8), :] = here
                    r[ROW_PAD + RATIO * y + j, h, pl.ds(COL_PAD + 8 * k, 8), :] = 0.8 / here
                    total = a if total is None else total + a
                sums[y, h, pl.ds(8 * k, 8), :] = total
        return carry
    lax.fori_loop(0, cy, prepare, 0)

    def keep_mass(y, h, g, total):
        cr[DEEP + y, h, pl.ds(COARSE_PAD + 8 * g, 8), :] = 0.8 / (4.0 + total)
    coarse_sums(sums, keep_mass)

    pl.semaphore_wait(barrier, len(around))
    for copy in u_loads:
        copy.wait()
    u0 = send("u0", ua, ua)
    for copy in f_loads:
        copy.wait()
    f2 = send("f", f, f)
    r2 = send("r", r, r)

    def sweep(src, dst, reach, starts, load, rate, top, count, step=2):
        def body(i, carry):
            y = top - reach + step * i
            for h in range(halves):
                for x in starts:
                    column = [at(src, y + j, h, x) for j in range(-1, step + 1)]
                    for j in range(step):
                        total = (column[j] + column[j + 2]) + (at(src, y + j, h, x - 1) + at(src, y + j, h, x + 1))
                        new = 0.2 * column[j + 1] + at(rate, y + j, h, x) * (at(load, y + j, h, x) + total)
                        dst[y + j, h, pl.ds(x, 8), :] = new
            return carry
        lax.fori_loop(0, (count + 2 * reach) // step, body, 0)

    arrived(u0)
    sweep(ua, ub, 0, own, f, r, ROW_PAD, ny)
    u1 = send("u1", ub, ub)
    coarse_mass = send("cr", cr, cr)
    f3 = send("f3", f, f)
    r3 = send("r3", r, r)
    for copy in u0:
        copy.wait_send()
    arrived(f2)
    arrived(r2)
    arrived(u1)
    sweep(ub, ua, 2, windows(COL_PAD, nx, 2), f, r, ROW_PAD, ny)
    sweep(ua, uc, 1, windows(COL_PAD, nx, 1), f, r, ROW_PAD, ny)

    def defect(y, carry):
        for h in range(halves):
            for k, x in enumerate(own):
                a, b, c, e = left_over(uc, f, d, ROW_PAD + RATIO * y, h, x)
                sums[y, h, pl.ds(8 * k, 8), :] = (a + b) + (c + e)
        return carry
    lax.fori_loop(0, cy, defect, 0)

    def keep_load(y, h, g, total):
        cl[DEEP + y, h, pl.ds(COARSE_PAD + 8 * g, 8), :] = total
    coarse_sums(sums, keep_load)
    coarse_load = send("cl", cl, cl)
    u3 = send("u3", uc, ud)

    arrived(coarse_mass)
    arrived(coarse_load)

    def first_coarse(y, carry):
        for h in range(halves):
            for x in windows(COARSE_PAD, cx, DEEP - 1):
                ca[y, h, pl.ds(x, 8), :] = at(cr, y, h, x) * at(cl, y, h, x)
        return carry
    lax.fori_loop(1, cy + 2 * DEEP - 1, first_coarse, 0)

    order = [ca, cb, ca, cb, cc, ca, cb, ca, cb]
    for k in range(1, INNER):
        reach = FIRST - 1 - k if k < FIRST else INNER - k
        if k == FIRST:
            arrived(send("cv", cc, cc))
        sweep(order[k - 1], order[k], reach, windows(COARSE_PAD, cx, reach), cl, cr, DEEP, cy)
    now = order[-1]

    def spread_row(y, carry):
        for h in range(halves):
            for w in range((cx + 2 + 7) // 8):
                c = at(now, DEEP - 1 + y, h, COARSE_PAD - 1 + 8 * w)
                for k in range(RATIO):
                    spread[y, h, pl.ds(32 * w + k, 8, stride=4), :] = c
        return carry
    lax.fori_loop(0, cy + 2, spread_row, 0)

    arrived(f3)
    arrived(r3)
    arrived(u3)

    def correct(y, carry):
        for h in range(halves):
            for x in windows(COL_PAD, nx, 1):
                add = spread[y, h, pl.ds(x - COL_PAD + 4, 8), :]
                for j in range(RATIO):
                    ua[RATIO * y + j, h, pl.ds(x, 8), :] = at(uc, RATIO * y + j, h, x) + add
            for x in (COL_PAD - 4, COL_PAD + nx + 1):
                add = spread[y, h, pl.ds(x - COL_PAD + 4, 3), :]
                for j in range(RATIO):
                    ua[RATIO * y + j, h, pl.ds(x, 3), :] = ud[RATIO * y + j, h, pl.ds(x, 3), :] + add
        return carry
    lax.fori_loop(1, cy + 1, correct, 0)

    for y in (0, cy + 1):
        def correct_edge(j, carry):
            for h in range(halves):
                for x in windows(COL_PAD, nx, 4):
                    add = spread[y, h, pl.ds(x - COL_PAD + 4, 8), :]
                    ua[RATIO * y + j, h, pl.ds(x, 8), :] = at(ud, RATIO * y + j, h, x) + add
            return carry
        lax.fori_loop(0, RATIO, correct_edge, 0)

    for y, row in ((0, ROW_PAD - 1), (cy + 1, ROW_PAD + ny)):
        for h in range(halves):
            for x in own:
                ua[row, h, pl.ds(x, 8), :] = at(uc, row, h, x) + spread[y, h, pl.ds(x - COL_PAD + 4, 8), :]

    for copy in u1:
        copy.wait_send()
    sweep(ua, ub, 3, windows(COL_PAD, nx, 3), f, r, ROW_PAD, ny)
    sweep(ub, ua, 2, windows(COL_PAD, nx, 2), f, r, ROW_PAD, ny)
    sweep(ua, ub, 1, windows(COL_PAD, nx, 1), f, r, ROW_PAD, ny)

    for name, made in sent:
        if name not in ("u0", "u1"):
            for copy in made:
                copy.wait_send()


def local(n_row, n_col, source_terms, initial_values, absorption):
    ny, nx, layers = source_terms.shape
    halves = layers // LANES
    sizes = (ny, nx, halves, n_row, n_col)
    _, _, count = plan(ny, nx)
    fine = (ny + 2 * ROW_PAD, halves, nx + 2 * COL_PAD, LANES)
    block = (ny, halves, nx, LANES)
    cy, cx = ny // RATIO, nx // RATIO
    coarse = pltpu.VMEM((cy + 2 * DEEP, halves, cx + 2 * COARSE_PAD, LANES), jnp.float32)

    def vmem(shape):
        return pltpu.VMEM(shape, jnp.float32)

    anywhere = pl.BlockSpec(memory_space=pltpu.HBM)
    inside = pl.BlockSpec(memory_space=pltpu.VMEM)
    u, f, d = pl.pallas_call(
        functools.partial(kernel, sizes),
        out_shape=(vmem(fine), vmem(fine), vmem(block)),
        in_specs=[anywhere] * 3,
        out_specs=(inside,) * 3,
        scratch_shapes=[
            vmem(fine), vmem(fine), vmem(fine), vmem(fine),
            vmem((cy, halves, nx, LANES)),
            vmem((cy + 2, halves, (cx + 8) * RATIO, LANES)),
            coarse, coarse, coarse, coarse, coarse,
            pltpu.SemaphoreType.DMA((3 * halves,)),
            pltpu.SemaphoreType.DMA((count,)),
            pltpu.SemaphoreType.DMA((count,)),
        ],
        compiler_params=pltpu.CompilerParams(
            collective_id=0, has_side_effects=True, vmem_limit_bytes=44_000_000
        ),
        name="two_grids",
    )(source_terms, initial_values, absorption)
    shape = jax.ShapeDtypeStruct(source_terms.shape, jnp.float32)
    return pl.pallas_call(
        functools.partial(finish, (ny, nx, halves)),
        out_shape=(shape, shape),
        in_specs=[inside] * 3,
        out_specs=(anywhere, anywhere),
        scratch_shapes=[vmem(block), pltpu.SemaphoreType.DMA((5 * halves,))],
        compiler_params=pltpu.CompilerParams(vmem_limit_bytes=8_000_000),
        name="finish",
    )(u, f, d)


def solution(mesh):
    n_row, n_col = mesh.shape["row"], mesh.shape["col"]
    spec = P("row", "col", None)
    return jax.shard_map(
        functools.partial(local, n_row, n_col),
        mesh=mesh, in_specs=(spec, spec, spec), out_specs=(spec, spec), check_vma=False,
    )
```

```python
import functools

import jax
import jax.numpy as jnp
from jax import lax
from jax.experimental import pallas as pl
from jax.experimental.pallas import tpu as pltpu
from jax.sharding import PartitionSpec as P

RATIO = 4
INNER = 9
LANES = 128
ROW_PAD = 4
COL_PAD = 8
FIRST = 5
DEEP = INNER - FIRST + 1
COARSE_PAD = 8
MESH = pl.DeviceIdType.MESH


def edge_rects(rows, cols, near, far):
    (y0, ny), (x0, nx) = rows, cols
    wide = far - near
    return [
        (0, 1, (y0, ny, x0 + nx - far, wide), (y0, ny, x0 - far, wide)),
        (0, -1, (y0, ny, x0 + near, wide), (y0, ny, x0 + nx + near, wide)),
        (1, 0, (y0 + ny - far, wide, x0, nx), (y0 - far, wide, x0, nx)),
        (-1, 0, (y0 + near, wide, x0, nx), (y0 + ny + near, wide, x0, nx)),
    ]


def corner_rects(rows, cols, near_y, far_y, far_x):
    (y0, ny), (x0, nx) = rows, cols
    wide = far_y - near_y
    found = []
    for dy in (1, -1):
        if dy == 1:
            from_y, to_y = y0 + ny - far_y, y0 - far_y
        else:
            from_y, to_y = y0 + near_y, y0 + ny + near_y
        for dx in (1, -1):
            if dx == 1:
                from_x, to_x = x0 + nx - far_x, x0 - far_x
            else:
                from_x, to_x = x0, x0 + nx
            found.append((dy, dx, (from_y, wide, from_x, far_x), (to_y, wide, to_x, far_x)))
    return found


def plan(ny, nx):
    rows, cols = (ROW_PAD, ny), (COL_PAD, nx)
    crows, ccols = (DEEP, ny // RATIO), (COARSE_PAD, nx // RATIO)
    coarse = edge_rects(crows, ccols, 0, DEEP - 1)
    coarse = coarse + corner_rects(crows, ccols, 0, 2, 4) + corner_rects(crows, ccols, 2, 4, 2)
    values = edge_rects(crows, ccols, 0, DEEP)
    values = values + corner_rects(crows, ccols, 0, 3, 5) + corner_rects(crows, ccols, 3, 5, 2)
    exchanges = {
        "u0": edge_rects(rows, cols, 0, 1),
        "f": edge_rects(rows, cols, 0, 2) + corner_rects(rows, cols, 0, 2, 2),
        "r": edge_rects(rows, cols, 0, 2) + corner_rects(rows, cols, 0, 2, 2),
        "u1": edge_rects(rows, cols, 0, 3) + corner_rects(rows, cols, 0, 2, 2),
        "cr": coarse,
        "f3": edge_rects(rows, cols, 2, 3),
        "r3": edge_rects(rows, cols, 2, 3),
        "cl": coarse,
        "u3": edge_rects(rows, cols, 1, 4) + corner_rects(rows, cols, 0, 3, 3),
        "cv": values,
    }
    at, first = 0, {}
    for name, rects in exchanges.items():
        first[name] = at
        at += len(rects)
    return exchanges, first, at


def left_over(u, f, d, y, h, x):
    column = [u[y + j, h, pl.ds(x, 8), :] for j in range(-1, RATIO + 1)]
    found = []
    for j in range(RATIO):
        beside = u[y + j, h, pl.ds(x - 1, 8), :] + u[y + j, h, pl.ds(x + 1, 8), :]
        total = f[y + j, h, pl.ds(x, 8), :] + ((column[j] + column[j + 2]) + beside)
        found.append(total - d[y + j - ROW_PAD, h, pl.ds(x - COL_PAD, 8), :] * column[j + 1])
    return found


def finish(sizes, u, f, d, improved_hbm, remaining_hbm, left, store_sem):
    ny, nx, halves = sizes
    cy = ny // RATIO

    def stores(k, ref, hbm, y0, x0, y, rows):
        made = []
        for h in range(halves):
            made.append(pltpu.make_async_copy(
                ref.at[pl.ds(y0 + y, rows), h, pl.ds(x0, nx), :],
                hbm.at[pl.ds(y, rows), :, pl.ds(h * LANES, LANES)],
                store_sem.at[k * halves + h]))
        for copy in made:
            copy.start()
        return made

    going = stores(0, u, improved_hbm, ROW_PAD, COL_PAD, 0, ny)
    parts = 4
    for part in range(parts):
        def remain(y, carry):
            for h in range(halves):
                for k in range(nx // 8):
                    for j, found in enumerate(left_over(u, f, d, ROW_PAD + RATIO * y, h, COL_PAD + 8 * k)):
                        left[RATIO * y + j, h, pl.ds(8 * k, 8), :] = found
            return carry
        lax.fori_loop(part * cy // parts, (part + 1) * cy // parts, remain, 0)
        going += stores(1 + part, left, remaining_hbm, 0, 0, part * ny // parts, ny // parts)
    for copy in going:
        copy.wait()


def kernel(sizes, f_hbm, u_hbm, a_hbm, ud, f, d,
           ua, ub, uc, r, sums, spread, cl, cr, ca, cb, cc,
           load_sem, send_sem, recv_sem):
    ny, nx, halves, n_row, n_col = sizes
    cy, cx = ny // RATIO, nx // RATIO
    exchanges, first, _ = plan(ny, nx)
    me_row, me_col = lax.axis_index("row"), lax.axis_index("col")

    def neighbour(dy, dx):
        return (lax.rem(me_row + dy + n_row, n_row), lax.rem(me_col + dx + n_col, n_col))

    def box(ref, where):
        y, h, x, w = where
        return ref.at[pl.ds(y, h), :, pl.ds(x, w), :]

    def copies(name, source, landing):
        made = []
        for k, (dy, dx, src, dst) in enumerate(exchanges[name]):
            made.append(pltpu.make_async_remote_copy(
                src_ref=box(source, src), dst_ref=box(landing, dst),
                send_sem=send_sem.at[first[name] + k], recv_sem=recv_sem.at[first[name] + k],
                device_id=neighbour(dy, dx), device_id_type=MESH))
        return made

    sent = []

    def send(name, source, landing):
        made = copies(name, source, landing)
        for copy in made:
            copy.start()
        sent.append((name, made))
        return made

    def arrived(made):
        for copy in made:
            copy.wait_recv()

    def loads(k, hbm, ref, y0, x0):
        made = []
        for h in range(halves):
            made.append(pltpu.make_async_copy(
                hbm.at[:, :, pl.ds(h * LANES, LANES)],
                ref.at[pl.ds(y0, ny), h, pl.ds(x0, nx), :],
                load_sem.at[k * halves + h]))
        for copy in made:
            copy.start()
        return made

    a_loads = loads(0, a_hbm, d, 0, 0)
    u_loads = loads(1, u_hbm, ua, ROW_PAD, COL_PAD)
    f_loads = loads(2, f_hbm, f, ROW_PAD, COL_PAD)

    barrier = pltpu.get_barrier_semaphore()
    around = [(dy, dx) for dy in (-1, 0, 1) for dx in (-1, 0, 1) if (dy, dx) != (0, 0)]
    for dy, dx in around:
        pl.semaphore_signal(barrier, inc=1, device_id=neighbour(dy, dx), device_id_type=MESH)

    own = [COL_PAD + 8 * k for k in range(nx // 8)]

    def windows(x0, n, reach):
        low, high = x0 - reach, x0 + n + reach
        return [min(x, high - 8) for x in range(low, high, 8)]

    def at(ref, y, h, x):
        return ref[y, h, pl.ds(x, 8), :]

    def coarse_sums(ref, done):
        def body(y, carry):
            for h in range(halves):
                for g in range(cx // 8):
                    parts = [sums[y, h, pl.ds(32 * g + k, 8, stride=4), :] for k in range(4)]
                    total = ((parts[0] + parts[1]) + (parts[2] + parts[3])) * 0.25
                    done(y, h, g, total)
            return carry
        lax.fori_loop(0, cy, body, 0)

    for copy in a_loads:
        copy.wait()

    def prepare(y, carry):
        for h in range(halves):
            for k in range(nx // 8):
                total = None
                for j in range(RATIO):
                    a = d[RATIO * y + j, h, pl.ds(8 * k, 8), :]
                    here = 4.0 + a
                    d[RATIO * y + j, h, pl.ds(8 * k, 8), :] = here
                    r[ROW_PAD + RATIO * y + j, h, pl.ds(COL_PAD + 8 * k, 8), :] = 0.8 / here
                    total = a if total is None else total + a
                sums[y, h, pl.ds(8 * k, 8), :] = total
        return carry
    lax.fori_loop(0, cy, prepare, 0)

    def keep_mass(y, h, g, total):
        cr[DEEP + y, h, pl.ds(COARSE_PAD + 8 * g, 8), :] = 0.8 / (4.0 + total)
    coarse_sums(sums, keep_mass)

    pl.semaphore_wait(barrier, len(around))
    for copy in u_loads:
        copy.wait()
    u0 = send("u0", ua, ua)
    for copy in f_loads:
        copy.wait()
    f2 = send("f", f, f)
    r2 = send("r", r, r)

    def region(src, dst, y0, y1, starts, load, rate):
        step = next(k for k in (2, 3, 1) if (y1 - y0) % k == 0)

        def body(i, carry):
            y = y0 + step * i
            for h in range(halves):
                for x in starts:
                    column = [at(src, y + j, h, x) for j in range(-1, step + 1)]
                    for j in range(step):
                        total = (column[j] + column[j + 2]) + (at(src, y + j, h, x - 1) + at(src, y + j, h, x + 1))
                        new = 0.2 * column[j + 1] + at(rate, y + j, h, x) * (at(load, y + j, h, x) + total)
                        dst[y + j, h, pl.ds(x, 8), :] = new
            return carry
        lax.fori_loop(0, (y1 - y0) // step, body, 0)

    def interior(src, dst, inset):
        region(src, dst, ROW_PAD + inset, ROW_PAD + ny - inset, windows(COL_PAD, nx, -inset), f, r)

    def frame(src, dst, inset, reach):
        low, high = ROW_PAD + inset, ROW_PAD + ny - inset
        full = windows(COL_PAD, nx, reach)
        region(src, dst, ROW_PAD - reach, low, full, f, r)
        region(src, dst, high, ROW_PAD + ny + reach, full, f, r)
        region(src, dst, low, high, [full[0], full[-1]], f, r)

    def defect(y0, y1, starts):
        def body(y, carry):
            for h in range(halves):
                for x in starts:
                    a, b, c, e = left_over(uc, f, d, ROW_PAD + RATIO * y, h, x)
                    sums[y, h, pl.ds(x - COL_PAD, 8), :] = (a + b) + (c + e)
            return carry
        lax.fori_loop(y0, y1, body, 0)

    interior(ua, ub, 1)
    arrived(u0)
    frame(ua, ub, 1, 0)
    u1 = send("u1", ub, ub)
    coarse_mass = send("cr", cr, cr)
    for copy in u0:
        copy.wait_send()

    interior(ub, ua, 1)
    interior(ua, uc, 2)
    defect(1, cy - 1, own[1:-1])
    arrived(f2)
    arrived(r2)
    arrived(u1)
    frame(ub, ua, 1, 2)
    frame(ua, uc, 2, 1)
    defect(0, 1, own)
    defect(cy - 1, cy, own)
    defect(1, cy - 1, [own[0], own[-1]])

    def keep_load(y, h, g, total):
        cl[DEEP + y, h, pl.ds(COARSE_PAD + 8 * g, 8), :] = total
    coarse_sums(sums, keep_load)
    coarse_load = send("cl", cl, cl)
    u3 = send("u3", uc, ud)

    arrived(coarse_mass)
    arrived(coarse_load)

    def first_coarse(y, carry):
        for h in range(halves):
            for x in windows(COARSE_PAD, cx, DEEP - 1):
                ca[y, h, pl.ds(x, 8), :] = at(cr, y, h, x) * at(cl, y, h, x)
        return carry
    lax.fori_loop(1, cy + 2 * DEEP - 1, first_coarse, 0)

    order = [ca, cb, ca, cb, cc, ca, cb, ca, cb]
    for k in range(1, INNER):
        reach = FIRST - 1 - k if k < FIRST else INNER - k
        if k == FIRST:
            coarse_values = send("cv", cc, cc)
            f3 = send("f3", f, f)
            r3 = send("r3", r, r)
            arrived(coarse_values)
        region(order[k - 1], order[k], DEEP - reach, DEEP + cy + reach, windows(COARSE_PAD, cx, reach), cl, cr)
    now = order[-1]

    def spread_row(y, carry):
        for h in range(halves):
            for w in range((cx + 2 + 7) // 8):
                c = at(now, DEEP - 1 + y, h, COARSE_PAD - 1 + 8 * w)
                for k in range(RATIO):
                    spread[y, h, pl.ds(32 * w + k, 8, stride=4), :] = c
        return carry
    lax.fori_loop(0, cy + 2, spread_row, 0)

    def correct(y, carry):
        for h in range(halves):
            for x in own:
                add = spread[y, h, pl.ds(x - COL_PAD + 4, 8), :]
                for j in range(RATIO):
                    ua[RATIO * y + j, h, pl.ds(x, 8), :] = at(uc, RATIO * y + j, h, x) + add
        return carry
    lax.fori_loop(1, cy + 1, correct, 0)

    for copy in u1:
        copy.wait_send()
    interior(ua, ub, 1)
    for copy in u3:
        copy.wait_send()
    interior(ub, uc, 2)
    interior(uc, ud, 3)

    arrived(u3)

    def correct_sides(y, carry):
        for h in range(halves):
            for x in (COL_PAD - 4, COL_PAD + nx + 1):
                add = spread[y, h, pl.ds(x - COL_PAD + 4, 3), :]
                for j in range(RATIO):
                    ua[RATIO * y + j, h, pl.ds(x, 3), :] = ud[RATIO * y + j, h, pl.ds(x, 3), :] + add
            for x in (COL_PAD - 1, COL_PAD + nx):
                add = spread[y, h, pl.ds(x - COL_PAD + 4, 1), :]
                for j in range(RATIO):
                    ua[RATIO * y + j, h, pl.ds(x, 1), :] = uc[RATIO * y + j, h, pl.ds(x, 1), :] + add
        return carry
    lax.fori_loop(1, cy + 1, correct_sides, 0)

    for y in (0, cy + 1):
        def correct_edge(j, carry):
            for h in range(halves):
                for x in windows(COL_PAD, nx, 4):
                    add = spread[y, h, pl.ds(x - COL_PAD + 4, 8), :]
                    ua[RATIO * y + j, h, pl.ds(x, 8), :] = at(ud, RATIO * y + j, h, x) + add
            return carry
        lax.fori_loop(0, RATIO, correct_edge, 0)

    for y, row in ((0, ROW_PAD - 1), (cy + 1, ROW_PAD + ny)):
        for h in range(halves):
            for x in own:
                ua[row, h, pl.ds(x, 8), :] = at(uc, row, h, x) + spread[y, h, pl.ds(x - COL_PAD + 4, 8), :]

    arrived(f3)
    arrived(r3)
    frame(ua, ub, 1, 3)
    frame(ub, uc, 2, 2)
    frame(uc, ud, 3, 1)

    for name, made in sent:
        if name not in ("u0", "u1", "u3"):
            for copy in made:
                copy.wait_send()


def local(n_row, n_col, source_terms, initial_values, absorption):
    ny, nx, layers = source_terms.shape
    halves = layers // LANES
    sizes = (ny, nx, halves, n_row, n_col)
    _, _, count = plan(ny, nx)
    fine = (ny + 2 * ROW_PAD, halves, nx + 2 * COL_PAD, LANES)
    block = (ny, halves, nx, LANES)
    cy, cx = ny // RATIO, nx // RATIO
    coarse = pltpu.VMEM((cy + 2 * DEEP, halves, cx + 2 * COARSE_PAD, LANES), jnp.float32)

    def vmem(shape):
        return pltpu.VMEM(shape, jnp.float32)

    anywhere = pl.BlockSpec(memory_space=pltpu.HBM)
    inside = pl.BlockSpec(memory_space=pltpu.VMEM)
    u, f, d = pl.pallas_call(
        functools.partial(kernel, sizes),
        out_shape=(vmem(fine), vmem(fine), vmem(block)),
        in_specs=[anywhere] * 3,
        out_specs=(inside,) * 3,
        scratch_shapes=[
            vmem(fine), vmem(fine), vmem(fine), vmem(fine),
            vmem((cy, halves, nx, LANES)),
            vmem((cy + 2, halves, (cx + 8) * RATIO, LANES)),
            coarse, coarse, coarse, coarse, coarse,
            pltpu.SemaphoreType.DMA((3 * halves,)),
            pltpu.SemaphoreType.DMA((count,)),
            pltpu.SemaphoreType.DMA((count,)),
        ],
        compiler_params=pltpu.CompilerParams(
            collective_id=0, has_side_effects=True, vmem_limit_bytes=44_000_000
        ),
        name="two_grids",
    )(source_terms, initial_values, absorption)
    shape = jax.ShapeDtypeStruct(source_terms.shape, jnp.float32)
    return pl.pallas_call(
        functools.partial(finish, (ny, nx, halves)),
        out_shape=(shape, shape),
        in_specs=[inside] * 3,
        out_specs=(anywhere, anywhere),
        scratch_shapes=[vmem(block), pltpu.SemaphoreType.DMA((5 * halves,))],
        compiler_params=pltpu.CompilerParams(vmem_limit_bytes=8_000_000),
        name="finish",
    )(u, f, d)


def solution(mesh):
    n_row, n_col = mesh.shape["row"], mesh.shape["col"]
    spec = P("row", "col", None)
    return jax.shard_map(
        functools.partial(local, n_row, n_col),
        mesh=mesh, in_specs=(spec, spec, spec), out_specs=(spec, spec), check_vma=False,
    )
```

```python
import functools

import jax
import jax.numpy as jnp
from jax import lax
from jax.experimental import pallas as pl
from jax.experimental.pallas import tpu as pltpu
from jax.sharding import PartitionSpec as P

RATIO = 4
INNER = 9
LANES = 128
ROW_PAD = 4
COL_PAD = 8
FIRST = 5
DEEP = INNER - FIRST + 1
COARSE_PAD = 8
MESH = pl.DeviceIdType.MESH


def edge_rects(rows, cols, near, far):
    (y0, ny), (x0, nx) = rows, cols
    wide = far - near
    return [
        (0, 1, (y0, ny, x0 + nx - far, wide), (y0, ny, x0 - far, wide)),
        (0, -1, (y0, ny, x0 + near, wide), (y0, ny, x0 + nx + near, wide)),
        (1, 0, (y0 + ny - far, wide, x0, nx), (y0 - far, wide, x0, nx)),
        (-1, 0, (y0 + near, wide, x0, nx), (y0 + ny + near, wide, x0, nx)),
    ]


def corner_rects(rows, cols, near_y, far_y, far_x):
    (y0, ny), (x0, nx) = rows, cols
    wide = far_y - near_y
    found = []
    for dy in (1, -1):
        if dy == 1:
            from_y, to_y = y0 + ny - far_y, y0 - far_y
        else:
            from_y, to_y = y0 + near_y, y0 + ny + near_y
        for dx in (1, -1):
            if dx == 1:
                from_x, to_x = x0 + nx - far_x, x0 - far_x
            else:
                from_x, to_x = x0, x0 + nx
            found.append((dy, dx, (from_y, wide, from_x, far_x), (to_y, wide, to_x, far_x)))
    return found


def plan(ny, nx):
    rows, cols = (ROW_PAD, ny), (COL_PAD, nx)
    crows, ccols = (DEEP, ny // RATIO), (COARSE_PAD, nx // RATIO)
    coarse = edge_rects(crows, ccols, 0, DEEP - 1)
    coarse = coarse + corner_rects(crows, ccols, 0, 2, 4) + corner_rects(crows, ccols, 2, 4, 2)
    values = edge_rects(crows, ccols, 0, DEEP)
    values = values + corner_rects(crows, ccols, 0, 3, 5) + corner_rects(crows, ccols, 3, 5, 2)
    exchanges = {
        "u0": edge_rects(rows, cols, 0, 2) + corner_rects(rows, cols, 0, 1, 1),
        "f": edge_rects(rows, cols, 0, 1),
        "r": edge_rects(rows, cols, 0, 1),
        "r3": edge_rects(rows, cols, 1, 3) + corner_rects(rows, cols, 0, 2, 2),
        "u2": edge_rects(rows, cols, 0, 2) + corner_rects(rows, cols, 0, 1, 1),
        "cr": coarse,
        "cl": coarse,
        "v4": edge_rects(rows, cols, 0, 2) + corner_rects(rows, cols, 0, 1, 1),
        "v6": edge_rects(rows, cols, 0, 1),
        "cv": values,
    }
    at, first = 0, {}
    for name, rects in exchanges.items():
        first[name] = at
        at += len(rects)
    return exchanges, first, at


def left_over(u, f, d, y, h, x):
    column = [u[y + j, h, pl.ds(x, 8), :] for j in range(-1, RATIO + 1)]
    found = []
    for j in range(RATIO):
        beside = u[y + j, h, pl.ds(x - 1, 8), :] + u[y + j, h, pl.ds(x + 1, 8), :]
        total = f[y + j, h, pl.ds(x, 8), :] + ((column[j] + column[j + 2]) + beside)
        found.append(total - d[y + j - ROW_PAD, h, pl.ds(x - COL_PAD, 8), :] * column[j + 1])
    return found


def finish(sizes, u, f, d, improved_hbm, remaining_hbm, left, store_sem):
    ny, nx, halves = sizes
    cy = ny // RATIO

    def stores(k, ref, hbm, y0, x0, y, rows):
        made = []
        for h in range(halves):
            made.append(pltpu.make_async_copy(
                ref.at[pl.ds(y0 + y, rows), h, pl.ds(x0, nx), :],
                hbm.at[pl.ds(y, rows), :, pl.ds(h * LANES, LANES)],
                store_sem.at[k * halves + h]))
        for copy in made:
            copy.start()
        return made

    going = stores(0, u, improved_hbm, ROW_PAD, COL_PAD, 0, ny)
    parts = 4
    for part in range(parts):
        def remain(y, carry):
            for h in range(halves):
                for k in range(nx // 8):
                    for j, found in enumerate(left_over(u, f, d, ROW_PAD + RATIO * y, h, COL_PAD + 8 * k)):
                        left[RATIO * y + j, h, pl.ds(8 * k, 8), :] = found
            return carry
        lax.fori_loop(part * cy // parts, (part + 1) * cy // parts, remain, 0)
        going += stores(1 + part, left, remaining_hbm, 0, 0, part * ny // parts, ny // parts)
    for copy in going:
        copy.wait()


def kernel(sizes, f_hbm, u_hbm, a_hbm, ua, f, d,
           ub, uc, ud, ue, r, sums, spread, cl, cr, ca, cb, cc,
           load_sem, send_sem, recv_sem):
    ny, nx, halves, n_row, n_col = sizes
    cy, cx = ny // RATIO, nx // RATIO
    exchanges, first, _ = plan(ny, nx)
    me_row, me_col = lax.axis_index("row"), lax.axis_index("col")

    def neighbour(dy, dx):
        return (lax.rem(me_row + dy + n_row, n_row), lax.rem(me_col + dx + n_col, n_col))

    def box(ref, where):
        y, h, x, w = where
        return ref.at[pl.ds(y, h), :, pl.ds(x, w), :]

    def copies(name, source, landing):
        made = []
        for k, (dy, dx, src, dst) in enumerate(exchanges[name]):
            made.append(pltpu.make_async_remote_copy(
                src_ref=box(source, src), dst_ref=box(landing, dst),
                send_sem=send_sem.at[first[name] + k], recv_sem=recv_sem.at[first[name] + k],
                device_id=neighbour(dy, dx), device_id_type=MESH))
        return made

    sent = []

    def send(name, source, landing):
        made = copies(name, source, landing)
        for copy in made:
            copy.start()
        sent.append((name, made))
        return made

    def arrived(made):
        for copy in made:
            copy.wait_recv()

    def loads(k, hbm, ref, y0, x0):
        made = []
        for h in range(halves):
            made.append(pltpu.make_async_copy(
                hbm.at[:, :, pl.ds(h * LANES, LANES)],
                ref.at[pl.ds(y0, ny), h, pl.ds(x0, nx), :],
                load_sem.at[k * halves + h]))
        for copy in made:
            copy.start()
        return made

    a_loads = loads(0, a_hbm, d, 0, 0)
    u_loads = loads(1, u_hbm, ua, ROW_PAD, COL_PAD)
    f_loads = loads(2, f_hbm, f, ROW_PAD, COL_PAD)

    barrier = pltpu.get_barrier_semaphore()
    around = [(dy, dx) for dy in (-1, 0, 1) for dx in (-1, 0, 1) if (dy, dx) != (0, 0)]
    for dy, dx in around:
        pl.semaphore_signal(barrier, inc=1, device_id=neighbour(dy, dx), device_id_type=MESH)

    own = [COL_PAD + 8 * k for k in range(nx // 8)]

    def windows(x0, n, reach):
        low, high = x0 - reach, x0 + n + reach
        return [min(x, high - 8) for x in range(low, high, 8)]

    def at(ref, y, h, x):
        return ref[y, h, pl.ds(x, 8), :]

    def coarse_sums(ref, done):
        def body(y, carry):
            for h in range(halves):
                for g in range(cx // 8):
                    parts = [sums[y, h, pl.ds(32 * g + k, 8, stride=4), :] for k in range(4)]
                    total = ((parts[0] + parts[1]) + (parts[2] + parts[3])) * 0.25
                    done(y, h, g, total)
            return carry
        lax.fori_loop(0, cy, body, 0)

    for copy in a_loads:
        copy.wait()

    def prepare(y, carry):
        for h in range(halves):
            for k in range(nx // 8):
                total = None
                for j in range(RATIO):
                    a = d[RATIO * y + j, h, pl.ds(8 * k, 8), :]
                    here = 4.0 + a
                    d[RATIO * y + j, h, pl.ds(8 * k, 8), :] = here
                    r[ROW_PAD + RATIO * y + j, h, pl.ds(COL_PAD + 8 * k, 8), :] = 0.8 / here
                    total = a if total is None else total + a
                sums[y, h, pl.ds(8 * k, 8), :] = total
        return carry
    lax.fori_loop(0, cy, prepare, 0)

    def keep_mass(y, h, g, total):
        cr[DEEP + y, h, pl.ds(COARSE_PAD + 8 * g, 8), :] = 0.8 / (4.0 + total)
    coarse_sums(sums, keep_mass)

    pl.semaphore_wait(barrier, len(around))
    for copy in u_loads:
        copy.wait()
    u0 = send("u0", ua, ua)
    for copy in f_loads:
        copy.wait()
    f1 = send("f", f, f)
    r1 = send("r", r, r)
    r3 = send("r3", r, r)

    def region(src, dst, y0, y1, starts, load, rate):
        step = next(k for k in (2, 3, 1) if (y1 - y0) % k == 0)

        def body(i, carry):
            y = y0 + step * i
            for h in range(halves):
                for x in starts:
                    column = [at(src, y + j, h, x) for j in range(-1, step + 1)]
                    for j in range(step):
                        total = (column[j] + column[j + 2]) + (at(src, y + j, h, x - 1) + at(src, y + j, h, x + 1))
                        new = 0.2 * column[j + 1] + at(rate, y + j, h, x) * (at(load, y + j, h, x) + total)
                        dst[y + j, h, pl.ds(x, 8), :] = new
            return carry
        lax.fori_loop(0, (y1 - y0) // step, body, 0)

    def interior(src, dst, inset):
        region(src, dst, ROW_PAD + inset, ROW_PAD + ny - inset, windows(COL_PAD, nx, -inset), f, r)

    def frame(src, dst, inset, reach):
        full = windows(COL_PAD, nx, reach)
        region(src, dst, ROW_PAD - reach, ROW_PAD + inset, own, f, r)
        region(src, dst, ROW_PAD + ny - inset, ROW_PAD + ny + reach, own, f, r)
        region(src, dst, ROW_PAD, ROW_PAD + ny, [full[0], full[-1]], f, r)

    def defect(y0, y1, starts):
        def body(y, carry):
            for h in range(halves):
                for x in starts:
                    a, b, c, e = left_over(ua, f, d, ROW_PAD + RATIO * y, h, x)
                    sums[y, h, pl.ds(x - COL_PAD, 8), :] = (a + b) + (c + e)
            return carry
        lax.fori_loop(y0, y1, body, 0)

    interior(ua, ub, 1)
    interior(ub, uc, 2)
    arrived(u0)
    arrived(f1)
    arrived(r1)
    frame(ua, ub, 1, 1)
    frame(ub, uc, 2, 0)
    u2 = send("u2", uc, uc)
    coarse_mass = send("cr", cr, cr)
    for copy in u0:
        copy.wait_send()

    interior(uc, ua, 1)
    defect(1, cy - 1, own[1:-1])
    interior(ua, ud, 2)
    arrived(u2)
    frame(uc, ua, 1, 1)
    defect(0, 1, own)
    defect(cy - 1, cy, own)
    defect(1, cy - 1, [own[0], own[-1]])

    def keep_load(y, h, g, total):
        cl[DEEP + y, h, pl.ds(COARSE_PAD + 8 * g, 8), :] = total
    coarse_sums(sums, keep_load)
    coarse_load = send("cl", cl, cl)
    frame(ua, ud, 2, 0)
    v4 = send("v4", ud, ud)

    interior(ud, ub, 1)
    interior(ub, ue, 2)

    arrived(coarse_mass)
    arrived(coarse_load)

    def first_coarse(y, carry):
        for h in range(halves):
            for x in windows(COARSE_PAD, cx, DEEP - 1):
                ca[y, h, pl.ds(x, 8), :] = at(cr, y, h, x) * at(cl, y, h, x)
        return carry
    lax.fori_loop(1, cy + 2 * DEEP - 1, first_coarse, 0)

    order = [ca, cb, ca, cb, cc, ca, cb, ca, cb]
    for k in range(1, INNER):
        reach = FIRST - 1 - k if k < FIRST else INNER - k
        if k == FIRST:
            coarse_values = send("cv", cc, cc)
            arrived(v4)
            frame(ud, ub, 1, 1)
            frame(ub, ue, 2, 0)
            v6 = send("v6", ue, ue)
            arrived(coarse_values)
        region(order[k - 1], order[k], DEEP - reach, DEEP + cy + reach, windows(COARSE_PAD, cx, reach), cl, cr)
    now = order[-1]

    def spread_row(y, carry):
        for h in range(halves):
            for w in range((cx + 2 + 7) // 8):
                c = at(now, DEEP - 1 + y, h, COARSE_PAD - 1 + 8 * w)
                for k in range(RATIO):
                    spread[y, h, pl.ds(32 * w + k, 8, stride=4), :] = c
        return carry
    lax.fori_loop(0, cy + 2, spread_row, 0)

    arrived(r3)
    for copy in u2:
        copy.wait_send()

    def swept(y, rows, starts):
        for h in range(halves):
            for x in starts:
                e = x - COL_PAD + 4
                here = spread[y, h, pl.ds(e, 8), :]
                beside = spread[y, h, pl.ds(e - 1, 8), :] + spread[y, h, pl.ds(e + 1, 8), :]
                kept = 0.2 * here
                for j in rows:
                    if j == 0:
                        total = beside + (here + spread[y - 1, h, pl.ds(e, 8), :])
                    elif j == RATIO - 1:
                        total = beside + (here + spread[y + 1, h, pl.ds(e, 8), :])
                    else:
                        total = beside + (here + here)
                    uc[RATIO * y + j, h, pl.ds(x, 8), :] = kept + at(r, RATIO * y + j, h, x) * total

    reach3 = windows(COL_PAD, nx, 3)

    def first_swept(y, carry):
        swept(y, range(RATIO), reach3)
        return carry
    lax.fori_loop(1, cy + 1, first_swept, 0)
    swept(0, range(1, RATIO), reach3)
    swept(cy + 1, range(RATIO - 1), reach3)

    def sweep_correction(src, dst, reach, base):
        starts = windows(COL_PAD, nx, reach)

        def body(i, carry):
            y = ROW_PAD - reach + 2 * i
            for h in range(halves):
                for x in starts:
                    column = [at(src, y + j, h, x) for j in range(-1, 3)]
                    for j in range(2):
                        total = (column[j] + column[j + 2]) + (at(src, y + j, h, x - 1) + at(src, y + j, h, x + 1))
                        new = 0.2 * column[j + 1] + at(r, y + j, h, x) * total
                        if base is not None:
                            new = at(base, y + j, h, x) + new
                        dst[y + j, h, pl.ds(x, 8), :] = new
            return carry
        lax.fori_loop(0, (ny + 2 * reach) // 2, body, 0)

    sweep_correction(uc, ub, 2, None)
    arrived(v6)
    sweep_correction(ub, ua, 1, ue)

    for name, made in sent:
        if name not in ("u0", "u2"):
            for copy in made:
                copy.wait_send()


def local(n_row, n_col, source_terms, initial_values, absorption):
    ny, nx, layers = source_terms.shape
    halves = layers // LANES
    sizes = (ny, nx, halves, n_row, n_col)
    _, _, count = plan(ny, nx)
    fine = (ny + 2 * ROW_PAD, halves, nx + 2 * COL_PAD, LANES)
    block = (ny, halves, nx, LANES)
    cy, cx = ny // RATIO, nx // RATIO
    coarse = pltpu.VMEM((cy + 2 * DEEP, halves, cx + 2 * COARSE_PAD, LANES), jnp.float32)

    def vmem(shape):
        return pltpu.VMEM(shape, jnp.float32)

    anywhere = pl.BlockSpec(memory_space=pltpu.HBM)
    inside = pl.BlockSpec(memory_space=pltpu.VMEM)
    u, f, d = pl.pallas_call(
        functools.partial(kernel, sizes),
        out_shape=(vmem(fine), vmem(fine), vmem(block)),
        in_specs=[anywhere] * 3,
        out_specs=(inside,) * 3,
        scratch_shapes=[
            vmem(fine), vmem(fine), vmem(fine), vmem(fine), vmem(fine),
            vmem((cy, halves, nx, LANES)),
            vmem((cy + 2, halves, (cx + 8) * RATIO, LANES)),
            coarse, coarse, coarse, coarse, coarse,
            pltpu.SemaphoreType.DMA((3 * halves,)),
            pltpu.SemaphoreType.DMA((count,)),
            pltpu.SemaphoreType.DMA((count,)),
        ],
        compiler_params=pltpu.CompilerParams(
            collective_id=0, has_side_effects=True, vmem_limit_bytes=44_000_000
        ),
        name="two_grids",
    )(source_terms, initial_values, absorption)
    shape = jax.ShapeDtypeStruct(source_terms.shape, jnp.float32)
    return pl.pallas_call(
        functools.partial(finish, (ny, nx, halves)),
        out_shape=(shape, shape),
        in_specs=[inside] * 3,
        out_specs=(anywhere, anywhere),
        scratch_shapes=[vmem(block), pltpu.SemaphoreType.DMA((5 * halves,))],
        compiler_params=pltpu.CompilerParams(vmem_limit_bytes=8_000_000),
        name="finish",
    )(u, f, d)


def solution(mesh):
    n_row, n_col = mesh.shape["row"], mesh.shape["col"]
    spec = P("row", "col", None)
    return jax.shard_map(
        functools.partial(local, n_row, n_col),
        mesh=mesh, in_specs=(spec, spec, spec), out_specs=(spec, spec), check_vma=False,
    )
```

```python
import functools

import jax
import jax.numpy as jnp
from jax import lax
from jax.experimental import pallas as pl
from jax.experimental.pallas import tpu as pltpu
from jax.sharding import PartitionSpec as P

RATIO = 4
INNER = 9
LANES = 128
ROW_PAD = 4
COL_PAD = 8
FIRST = 5
DEEP = INNER - FIRST + 1
COARSE_PAD = 8
MESH = pl.DeviceIdType.MESH


def edge_rects(rows, cols, near, far):
    (y0, ny), (x0, nx) = rows, cols
    wide = far - near
    return [
        (0, 1, (y0, ny, x0 + nx - far, wide), (y0, ny, x0 - far, wide)),
        (0, -1, (y0, ny, x0 + near, wide), (y0, ny, x0 + nx + near, wide)),
        (1, 0, (y0 + ny - far, wide, x0, nx), (y0 - far, wide, x0, nx)),
        (-1, 0, (y0 + near, wide, x0, nx), (y0 + ny + near, wide, x0, nx)),
    ]


def corner_rects(rows, cols, near_y, far_y, far_x):
    (y0, ny), (x0, nx) = rows, cols
    wide = far_y - near_y
    found = []
    for dy in (1, -1):
        if dy == 1:
            from_y, to_y = y0 + ny - far_y, y0 - far_y
        else:
            from_y, to_y = y0 + near_y, y0 + ny + near_y
        for dx in (1, -1):
            if dx == 1:
                from_x, to_x = x0 + nx - far_x, x0 - far_x
            else:
                from_x, to_x = x0, x0 + nx
            found.append((dy, dx, (from_y, wide, from_x, far_x), (to_y, wide, to_x, far_x)))
    return found


def plan(ny, nx):
    rows, cols = (ROW_PAD, ny), (COL_PAD, nx)
    crows, ccols = (DEEP, ny // RATIO), (COARSE_PAD, nx // RATIO)
    coarse = edge_rects(crows, ccols, 0, DEEP - 1)
    coarse = coarse + corner_rects(crows, ccols, 0, 2, 4) + corner_rects(crows, ccols, 2, 4, 2)
    values = edge_rects(crows, ccols, 0, DEEP)
    values = values + corner_rects(crows, ccols, 0, 3, 5) + corner_rects(crows, ccols, 3, 5, 2)
    exchanges = {
        "u0": edge_rects(rows, cols, 0, 2) + corner_rects(rows, cols, 0, 1, 1),
        "f": edge_rects(rows, cols, 0, 1),
        "r": edge_rects(rows, cols, 0, 1),
        "r3": edge_rects(rows, cols, 1, 3) + corner_rects(rows, cols, 0, 2, 2),
        "u2": edge_rects(rows, cols, 0, 2) + corner_rects(rows, cols, 0, 1, 1),
        "cr": coarse,
        "cl": coarse,
        "v4": edge_rects(rows, cols, 0, 2) + corner_rects(rows, cols, 0, 1, 1),
        "v6": edge_rects(rows, cols, 0, 1),
        "cv": values,
    }
    at, first = 0, {}
    for name, rects in exchanges.items():
        first[name] = at
        at += len(rects)
    return exchanges, first, at


def left_over(u, f, d, y, h, x):
    column = [u[y + j, h, pl.ds(x, 8), :] for j in range(-1, RATIO + 1)]
    found = []
    for j in range(RATIO):
        beside = u[y + j, h, pl.ds(x - 1, 8), :] + u[y + j, h, pl.ds(x + 1, 8), :]
        total = f[y + j, h, pl.ds(x, 8), :] + ((column[j] + column[j + 2]) + beside)
        found.append(total - d[y + j - ROW_PAD, h, pl.ds(x - COL_PAD, 8), :] * column[j + 1])
    return found


def windows(x0, n, reach):
    low, high = x0 - reach, x0 + n + reach
    return [min(x, high - 8) for x in range(low, high, 8)]


def swept_twice(src, r, base, dst, y, h, x):
    column = [src[y + j, h, pl.ds(x, 8), :] for j in range(-1, 3)]
    for j in range(2):
        beside = src[y + j, h, pl.ds(x - 1, 8), :] + src[y + j, h, pl.ds(x + 1, 8), :]
        total = (column[j] + column[j + 2]) + beside
        new = 0.2 * column[j + 1] + r[y + j, h, pl.ds(x, 8), :] * total
        if base is not None:
            new = base[y + j, h, pl.ds(x, 8), :] + new
        dst[y + j, h, pl.ds(x, 8), :] = new


def finish(sizes, e, v, f, d, r, improved_hbm, remaining_hbm, u, left, store_sem):
    ny, nx, halves = sizes
    cy = ny // RATIO

    def stores(k, ref, hbm, y0, x0, y, rows):
        made = []
        for h in range(halves):
            made.append(pltpu.make_async_copy(
                ref.at[pl.ds(y0 + y, rows), h, pl.ds(x0, nx), :],
                hbm.at[pl.ds(y, rows), :, pl.ds(h * LANES, LANES)],
                store_sem.at[k * halves + h]))
        for copy in made:
            copy.start()
        return made

    going = []
    parts = 4
    starts = windows(COL_PAD, nx, 1)
    rows = ny // parts
    for part in range(parts):
        low = part * rows + 1 if part else -1

        def last(i, carry):
            for h in range(halves):
                for x in starts:
                    swept_twice(e, r, v, u, ROW_PAD + low + 2 * i, h, x)
            return carry
        lax.fori_loop(0, ((part + 1) * rows + 1 - low) // 2, last, 0)
        going += stores(2 * part, u, improved_hbm, ROW_PAD, COL_PAD, part * rows, rows)

        def remain(y, carry):
            for h in range(halves):
                for k in range(nx // 8):
                    for j, found in enumerate(left_over(u, f, d, ROW_PAD + RATIO * y, h, COL_PAD + 8 * k)):
                        left[RATIO * y + j, h, pl.ds(8 * k, 8), :] = found
            return carry
        lax.fori_loop(part * cy // parts, (part + 1) * cy // parts, remain, 0)
        going += stores(2 * part + 1, left, remaining_hbm, 0, 0, part * ny // parts, ny // parts)
    for copy in going:
        copy.wait()


def kernel(sizes, f_hbm, u_hbm, a_hbm, ub, ue, f, d, r,
           ua, uc, ud, sums, spread, cl, cr, ca, cb, cc,
           load_sem, send_sem, recv_sem):
    ny, nx, halves, n_row, n_col = sizes
    cy, cx = ny // RATIO, nx // RATIO
    exchanges, first, _ = plan(ny, nx)
    me_row, me_col = lax.axis_index("row"), lax.axis_index("col")

    def neighbour(dy, dx):
        return (lax.rem(me_row + dy + n_row, n_row), lax.rem(me_col + dx + n_col, n_col))

    def box(ref, where):
        y, h, x, w = where
        return ref.at[pl.ds(y, h), :, pl.ds(x, w), :]

    def copies(name, source, landing):
        made = []
        for k, (dy, dx, src, dst) in enumerate(exchanges[name]):
            made.append((pltpu.make_async_remote_copy(
                src_ref=box(source, src), dst_ref=box(landing, dst),
                send_sem=send_sem.at[first[name] + k], recv_sem=recv_sem.at[first[name] + k],
                device_id=neighbour(dy, dx), device_id_type=MESH), dx == 0))
        return made

    sent = []

    def send(*given):
        found = [copies(*one) for one in given]
        sent.extend(found)
        return found

    def along(made, y_only):
        return [copy for part in made for copy, is_y in part if is_y == y_only]

    def start_x(made):
        for copy in along(made, False):
            copy.start()

    def start_y(made):
        for copy in along(made, True):
            copy.start()

    def gone_x(made):
        for copy in along(made, False):
            copy.wait_send()

    def gone_y(made):
        for copy in along(made, True):
            copy.wait_send()

    def arrived(made):
        for part in made:
            for copy, _ in part:
                copy.wait_recv()

    barrier = pltpu.get_barrier_semaphore()
    around = [(dy, dx) for dy in (-1, 0, 1) for dx in (-1, 0, 1) if (dy, dx) != (0, 0)]
    for dy, dx in around:
        pl.semaphore_signal(barrier, inc=1, device_id=neighbour(dy, dx), device_id_type=MESH)

    def loads(k, hbm, ref, y0, x0):
        made = []
        for h in range(halves):
            made.append(pltpu.make_async_copy(
                hbm.at[:, :, pl.ds(h * LANES, LANES)],
                ref.at[pl.ds(y0, ny), h, pl.ds(x0, nx), :],
                load_sem.at[k * halves + h]))
        for copy in made:
            copy.start()
        return made

    a_loads = loads(0, a_hbm, d, 0, 0)
    u_loads = loads(1, u_hbm, ua, ROW_PAD, COL_PAD)
    f_loads = loads(2, f_hbm, f, ROW_PAD, COL_PAD)

    own = [COL_PAD + 8 * k for k in range(nx // 8)]

    def at(ref, y, h, x):
        return ref[y, h, pl.ds(x, 8), :]

    def coarse_sums(ref, done):
        def body(y, carry):
            for h in range(halves):
                for g in range(cx // 8):
                    parts = [sums[y, h, pl.ds(32 * g + k, 8, stride=4), :] for k in range(4)]
                    total = ((parts[0] + parts[1]) + (parts[2] + parts[3])) * 0.25
                    done(y, h, g, total)
            return carry
        lax.fori_loop(0, cy, body, 0)

    for copy in a_loads:
        copy.wait()

    def prepare(y, carry):
        for h in range(halves):
            for k in range(nx // 8):
                total = None
                for j in range(RATIO):
                    a = d[RATIO * y + j, h, pl.ds(8 * k, 8), :]
                    here = 4.0 + a
                    d[RATIO * y + j, h, pl.ds(8 * k, 8), :] = here
                    r[ROW_PAD + RATIO * y + j, h, pl.ds(COL_PAD + 8 * k, 8), :] = 0.8 / here
                    total = a if total is None else total + a
                sums[y, h, pl.ds(8 * k, 8), :] = total
        return carry
    lax.fori_loop(0, cy, prepare, 0)

    def keep_mass(y, h, g, total):
        cr[DEEP + y, h, pl.ds(COARSE_PAD + 8 * g, 8), :] = 0.8 / (4.0 + total)
    coarse_sums(sums, keep_mass)

    pl.semaphore_wait(barrier, len(around))
    for copy in u_loads:
        copy.wait()
    for copy in f_loads:
        copy.wait()
    start = send(("u0", ua, ua), ("f", f, f), ("r", r, r))
    start_x(start)

    def region(src, dst, y0, y1, starts, load, rate):
        step = next(k for k in (2, 3, 1) if (y1 - y0) % k == 0)

        def body(i, carry):
            y = y0 + step * i
            for h in range(halves):
                for x in starts:
                    column = [at(src, y + j, h, x) for j in range(-1, step + 1)]
                    for j in range(step):
                        total = (column[j] + column[j + 2]) + (at(src, y + j, h, x - 1) + at(src, y + j, h, x + 1))
                        new = 0.2 * column[j + 1] + at(rate, y + j, h, x) * (at(load, y + j, h, x) + total)
                        dst[y + j, h, pl.ds(x, 8), :] = new
            return carry
        lax.fori_loop(0, (y1 - y0) // step, body, 0)

    def interior(src, dst, inset):
        region(src, dst, ROW_PAD + inset, ROW_PAD + ny - inset, windows(COL_PAD, nx, -inset), f, r)

    def frame(src, dst, inset, reach):
        full = windows(COL_PAD, nx, reach)
        region(src, dst, ROW_PAD - reach, ROW_PAD + inset, own, f, r)
        region(src, dst, ROW_PAD + ny - inset, ROW_PAD + ny + reach, own, f, r)
        region(src, dst, ROW_PAD, ROW_PAD + ny, [full[0], full[-1]], f, r)

    def defect(y0, y1, starts):
        def body(y, carry):
            for h in range(halves):
                for x in starts:
                    a, b, c, e = left_over(ua, f, d, ROW_PAD + RATIO * y, h, x)
                    sums[y, h, pl.ds(x - COL_PAD, 8), :] = (a + b) + (c + e)
            return carry
        lax.fori_loop(y0, y1, body, 0)

    interior(ua, ub, 1)
    interior(ub, uc, 2)
    gone_x(start)
    start_y(start)
    r3 = send(("r3", r, r))
    gone_y(start)
    start_x(r3)
    arrived(start)
    frame(ua, ub, 1, 1)
    frame(ub, uc, 2, 0)
    u2 = send(("u2", uc, uc))
    start_x(u2)

    interior(uc, ua, 1)
    defect(1, cy - 1, own[1:-1])
    gone_x(u2)
    start_y(u2)
    coarse_mass = send(("cr", cr, cr))
    start_x(coarse_mass)
    start_y(coarse_mass)
    start_y(r3)
    interior(ua, ud, 2)
    arrived(u2)
    frame(uc, ua, 1, 1)
    defect(0, 1, own)
    defect(cy - 1, cy, own)
    defect(1, cy - 1, [own[0], own[-1]])

    def keep_load(y, h, g, total):
        cl[DEEP + y, h, pl.ds(COARSE_PAD + 8 * g, 8), :] = total
    coarse_sums(sums, keep_load)
    coarse_load = send(("cl", cl, cl))
    start_x(coarse_load)
    frame(ua, ud, 2, 0)

    interior(ud, ub, 1)
    gone_x(coarse_load)
    start_y(coarse_load)
    v4 = send(("v4", ud, ud))
    start_x(v4)
    start_y(v4)
    interior(ub, ue, 2)

    arrived(coarse_mass)
    arrived(coarse_load)

    def first_coarse(y, carry):
        for h in range(halves):
            for x in windows(COARSE_PAD, cx, DEEP - 1):
                ca[y, h, pl.ds(x, 8), :] = at(cr, y, h, x) * at(cl, y, h, x)
        return carry
    lax.fori_loop(1, cy + 2 * DEEP - 1, first_coarse, 0)

    order = [ca, cb, ca, cb, cc, ca, cb, ca, cb]
    for k in range(1, INNER):
        reach = FIRST - 1 - k if k < FIRST else INNER - k
        if k == FIRST:
            coarse_values = send(("cv", cc, cc))
            start_x(coarse_values)
            gone_x(coarse_values)
            start_y(coarse_values)
            arrived(v4)
            frame(ud, ub, 1, 1)
            frame(ub, ue, 2, 0)
            v6 = send(("v6", ue, ue))
            start_x(v6)
            start_y(v6)
            arrived(coarse_values)
        region(order[k - 1], order[k], DEEP - reach, DEEP + cy + reach, windows(COARSE_PAD, cx, reach), cl, cr)
    now = order[-1]

    def spread_row(y, carry):
        for h in range(halves):
            for w in range((cx + 2 + 7) // 8):
                c = at(now, DEEP - 1 + y, h, COARSE_PAD - 1 + 8 * w)
                for k in range(RATIO):
                    spread[y, h, pl.ds(32 * w + k, 8, stride=4), :] = c
        return carry
    lax.fori_loop(0, cy + 2, spread_row, 0)

    arrived(r3)
    gone_y(u2)

    def swept(y, rows, starts):
        for h in range(halves):
            for x in starts:
                e = x - COL_PAD + 4
                here = spread[y, h, pl.ds(e, 8), :]
                beside = spread[y, h, pl.ds(e - 1, 8), :] + spread[y, h, pl.ds(e + 1, 8), :]
                kept = 0.2 * here
                for j in rows:
                    if j == 0:
                        total = beside + (here + spread[y - 1, h, pl.ds(e, 8), :])
                    elif j == RATIO - 1:
                        total = beside + (here + spread[y + 1, h, pl.ds(e, 8), :])
                    else:
                        total = beside + (here + here)
                    uc[RATIO * y + j, h, pl.ds(x, 8), :] = kept + at(r, RATIO * y + j, h, x) * total

    reach3 = windows(COL_PAD, nx, 3)

    def first_swept(y, carry):
        swept(y, range(RATIO), reach3)
        return carry
    lax.fori_loop(1, cy + 1, first_swept, 0)
    swept(0, range(1, RATIO), reach3)
    swept(cy + 1, range(RATIO - 1), reach3)

    starts = windows(COL_PAD, nx, 2)

    def second_swept(i, carry):
        for h in range(halves):
            for x in starts:
                swept_twice(uc, r, None, ub, ROW_PAD - 2 + 2 * i, h, x)
        return carry
    lax.fori_loop(0, (ny + 4) // 2, second_swept, 0)
    arrived(v6)

    for made in (r3, coarse_mass, coarse_load, v4, coarse_values, v6):
        if made is not coarse_load and made is not coarse_values:
            gone_x(made)
        gone_y(made)


def local(n_row, n_col, source_terms, initial_values, absorption):
    ny, nx, layers = source_terms.shape
    halves = layers // LANES
    sizes = (ny, nx, halves, n_row, n_col)
    _, _, count = plan(ny, nx)
    fine = (ny + 2 * ROW_PAD, halves, nx + 2 * COL_PAD, LANES)
    block = (ny, halves, nx, LANES)
    cy, cx = ny // RATIO, nx // RATIO
    coarse = pltpu.VMEM((cy + 2 * DEEP, halves, cx + 2 * COARSE_PAD, LANES), jnp.float32)

    def vmem(shape):
        return pltpu.VMEM(shape, jnp.float32)

    anywhere = pl.BlockSpec(memory_space=pltpu.HBM)
    inside = pl.BlockSpec(memory_space=pltpu.VMEM)
    held = pl.pallas_call(
        functools.partial(kernel, sizes),
        out_shape=(vmem(fine), vmem(fine), vmem(fine), vmem(block), vmem(fine)),
        in_specs=[anywhere] * 3,
        out_specs=(inside,) * 5,
        scratch_shapes=[
            vmem(fine), vmem(fine), vmem(fine),
            vmem((cy, halves, nx, LANES)),
            vmem((cy + 2, halves, (cx + 8) * RATIO, LANES)),
            coarse, coarse, coarse, coarse, coarse,
            pltpu.SemaphoreType.DMA((3 * halves,)),
            pltpu.SemaphoreType.DMA((count,)),
            pltpu.SemaphoreType.DMA((count,)),
        ],
        compiler_params=pltpu.CompilerParams(
            collective_id=0, has_side_effects=True, vmem_limit_bytes=25_300_000
        ),
        name="two_grids",
    )(source_terms, initial_values, absorption)
    shape = jax.ShapeDtypeStruct(source_terms.shape, jnp.float32)
    return pl.pallas_call(
        functools.partial(finish, (ny, nx, halves)),
        out_shape=(shape, shape),
        in_specs=[inside] * 5,
        out_specs=(anywhere, anywhere),
        scratch_shapes=[vmem(fine), vmem(block), pltpu.SemaphoreType.DMA((8 * halves,))],
        compiler_params=pltpu.CompilerParams(vmem_limit_bytes=14_000_000),
        name="finish",
    )(*held)


def solution(mesh):
    n_row, n_col = mesh.shape["row"], mesh.shape["col"]
    spec = P("row", "col", None)
    return jax.shard_map(
        functools.partial(local, n_row, n_col),
        mesh=mesh, in_specs=(spec, spec, spec), out_specs=(spec, spec), check_vma=False,
    )
```

```python
import functools

import jax
import jax.numpy as jnp
from jax import lax
from jax.experimental import pallas as pl
from jax.experimental.pallas import tpu as pltpu
from jax.sharding import PartitionSpec as P

RATIO = 4
INNER = 9
LANES = 128
ROW_PAD = 4
COL_PAD = 8
FIRST = 5
DEEP = INNER - FIRST + 1
COARSE_PAD = 8
MESH = pl.DeviceIdType.MESH


def edge_rects(rows, cols, near, far):
    (y0, ny), (x0, nx) = rows, cols
    wide = far - near
    return [
        (0, 1, (y0, ny, x0 + nx - far, wide), (y0, ny, x0 - far, wide)),
        (0, -1, (y0, ny, x0 + near, wide), (y0, ny, x0 + nx + near, wide)),
        (1, 0, (y0 + ny - far, wide, x0, nx), (y0 - far, wide, x0, nx)),
        (-1, 0, (y0 + near, wide, x0, nx), (y0 + ny + near, wide, x0, nx)),
    ]


def corner_rects(rows, cols, near_y, far_y, far_x):
    (y0, ny), (x0, nx) = rows, cols
    wide = far_y - near_y
    found = []
    for dy in (1, -1):
        if dy == 1:
            from_y, to_y = y0 + ny - far_y, y0 - far_y
        else:
            from_y, to_y = y0 + near_y, y0 + ny + near_y
        for dx in (1, -1):
            if dx == 1:
                from_x, to_x = x0 + nx - far_x, x0 - far_x
            else:
                from_x, to_x = x0, x0 + nx
            found.append((dy, dx, (from_y, wide, from_x, far_x), (to_y, wide, to_x, far_x)))
    return found


def plan(ny, nx):
    rows, cols = (ROW_PAD, ny), (COL_PAD, nx)
    crows, ccols = (DEEP, ny // RATIO), (COARSE_PAD, nx // RATIO)
    coarse = edge_rects(crows, ccols, 0, DEEP - 1)
    coarse = coarse + corner_rects(crows, ccols, 0, 2, 4) + corner_rects(crows, ccols, 2, 4, 2)
    values = edge_rects(crows, ccols, 0, DEEP)
    values = values + corner_rects(crows, ccols, 0, 3, 5) + corner_rects(crows, ccols, 3, 5, 2)
    exchanges = {
        "u0": edge_rects(rows, cols, 0, 2) + corner_rects(rows, cols, 0, 1, 1),
        "f": edge_rects(rows, cols, 0, 1),
        "r": edge_rects(rows, cols, 0, 1),
        "r3": edge_rects(rows, cols, 1, 3) + corner_rects(rows, cols, 0, 2, 2),
        "u2": edge_rects(rows, cols, 0, 2) + corner_rects(rows, cols, 0, 1, 1),
        "cr": coarse,
        "cl": coarse,
        "v4": edge_rects(rows, cols, 0, 2) + corner_rects(rows, cols, 0, 1, 1),
        "v6": edge_rects(rows, cols, 0, 1),
        "cv": values,
    }
    at, first = 0, {}
    for name, rects in exchanges.items():
        first[name] = at
        at += len(rects)
    return exchanges, first, at


def left_over(u, f, d, y, h, x):
    column = [u[y + j, h, pl.ds(x, 8), :] for j in range(-1, RATIO + 1)]
    found = []
    for j in range(RATIO):
        beside = u[y + j, h, pl.ds(x - 1, 8), :] + u[y + j, h, pl.ds(x + 1, 8), :]
        total = f[y + j, h, pl.ds(x, 8), :] + ((column[j] + column[j + 2]) + beside)
        found.append(total - d[y + j - ROW_PAD, h, pl.ds(x - COL_PAD, 8), :] * column[j + 1])
    return found


def windows(x0, n, reach):
    low, high = x0 - reach, x0 + n + reach
    return [min(x, high - 8) for x in range(low, high, 8)]


def swept_twice(src, r, base, dst, y, h, x):
    column = [src[y + j, h, pl.ds(x, 8), :] for j in range(-1, 3)]
    for j in range(2):
        beside = src[y + j, h, pl.ds(x - 1, 8), :] + src[y + j, h, pl.ds(x + 1, 8), :]
        total = (column[j] + column[j + 2]) + beside
        new = 0.2 * column[j + 1] + r[y + j, h, pl.ds(x, 8), :] * total
        if base is not None:
            new = base[y + j, h, pl.ds(x, 8), :] + new
        dst[y + j, h, pl.ds(x, 8), :] = new


def finish(sizes, e, v, f, d, r, improved_hbm, remaining_hbm, u, left, store_sem):
    ny, nx, halves = sizes
    cy = ny // RATIO

    def stores(k, ref, hbm, y0, x0, y, rows):
        made = []
        for h in range(halves):
            made.append(pltpu.make_async_copy(
                ref.at[pl.ds(y0 + y, rows), h, pl.ds(x0, nx), :],
                hbm.at[pl.ds(y, rows), :, pl.ds(h * LANES, LANES)],
                store_sem.at[k * halves + h]))
        for copy in made:
            copy.start()
        return made

    going = []
    parts = 4
    starts = windows(COL_PAD, nx, 1)
    rows = ny // parts
    for part in range(parts):
        low = part * rows + 1 if part else -1

        def last(i, carry):
            for h in range(halves):
                for x in starts:
                    swept_twice(e, r, v, u, ROW_PAD + low + 2 * i, h, x)
            return carry
        lax.fori_loop(0, ((part + 1) * rows + 1 - low) // 2, last, 0)
        going += stores(2 * part, u, improved_hbm, ROW_PAD, COL_PAD, part * rows, rows)

        def remain(y, carry):
            for h in range(halves):
                for k in range(nx // 8):
                    for j, found in enumerate(left_over(u, f, d, ROW_PAD + RATIO * y, h, COL_PAD + 8 * k)):
                        left[RATIO * y + j, h, pl.ds(8 * k, 8), :] = found
            return carry
        lax.fori_loop(part * cy // parts, (part + 1) * cy // parts, remain, 0)
        going += stores(2 * part + 1, left, remaining_hbm, 0, 0, part * ny // parts, ny // parts)
    for copy in going:
        copy.wait()


def kernel(sizes, f_hbm, u_hbm, a_hbm, ub, ue, f, d, r,
           ua, uc, ud, sums, spread, cl, cr, ca, cb, cc,
           load_sem, send_sem, recv_sem):
    ny, nx, halves, n_row, n_col = sizes
    cy, cx = ny // RATIO, nx // RATIO
    exchanges, first, _ = plan(ny, nx)
    me_row, me_col = lax.axis_index("row"), lax.axis_index("col")

    def neighbour(dy, dx):
        return (lax.rem(me_row + dy + n_row, n_row), lax.rem(me_col + dx + n_col, n_col))

    def box(ref, where):
        y, h, x, w = where
        return ref.at[pl.ds(y, h), :, pl.ds(x, w), :]

    def copies(name, source, landing):
        made = []
        for k, (dy, dx, src, dst) in enumerate(exchanges[name]):
            made.append((pltpu.make_async_remote_copy(
                src_ref=box(source, src), dst_ref=box(landing, dst),
                send_sem=send_sem.at[first[name] + k], recv_sem=recv_sem.at[first[name] + k],
                device_id=neighbour(dy, dx), device_id_type=MESH), dx == 0))
        return made

    def send(*given):
        return [copies(*one) for one in given]

    def start_along(made, y_only):
        for part in made:
            for copy, is_y in part:
                if is_y == y_only:
                    copy.start()

    def start(made):
        start_along(made, False)
        start_along(made, True)
        return made

    def gone(made):
        for part in made:
            for copy, _ in part:
                copy.wait_send()

    def arrived(made):
        for part in made:
            for copy, _ in part:
                copy.wait_recv()

    barrier = pltpu.get_barrier_semaphore()
    around = [(dy, dx) for dy in (-1, 0, 1) for dx in (-1, 0, 1) if (dy, dx) != (0, 0)]
    for dy, dx in around:
        pl.semaphore_signal(barrier, inc=1, device_id=neighbour(dy, dx), device_id_type=MESH)

    def loads(k, hbm, ref, y0, x0):
        made = []
        for h in range(halves):
            made.append(pltpu.make_async_copy(
                hbm.at[:, :, pl.ds(h * LANES, LANES)],
                ref.at[pl.ds(y0, ny), h, pl.ds(x0, nx), :],
                load_sem.at[k * halves + h]))
        for copy in made:
            copy.start()
        return made

    a_loads = loads(0, a_hbm, d, 0, 0)
    u_loads = loads(1, u_hbm, ua, ROW_PAD, COL_PAD)
    f_loads = loads(2, f_hbm, f, ROW_PAD, COL_PAD)

    own = [COL_PAD + 8 * k for k in range(nx // 8)]

    def at(ref, y, h, x):
        return ref[y, h, pl.ds(x, 8), :]

    def coarse_sums(ref, done):
        def body(y, carry):
            for h in range(halves):
                for g in range(cx // 8):
                    parts = [sums[y, h, pl.ds(32 * g + k, 8, stride=4), :] for k in range(4)]
                    total = ((parts[0] + parts[1]) + (parts[2] + parts[3])) * 0.25
                    done(y, h, g, total)
            return carry
        lax.fori_loop(0, cy, body, 0)

    for copy in a_loads:
        copy.wait()

    def prepare(y, carry):
        for h in range(halves):
            for k in range(nx // 8):
                total = None
                for j in range(RATIO):
                    a = d[RATIO * y + j, h, pl.ds(8 * k, 8), :]
                    here = 4.0 + a
                    d[RATIO * y + j, h, pl.ds(8 * k, 8), :] = here
                    r[ROW_PAD + RATIO * y + j, h, pl.ds(COL_PAD + 8 * k, 8), :] = 0.8 / here
                    total = a if total is None else total + a
                sums[y, h, pl.ds(8 * k, 8), :] = total
        return carry
    lax.fori_loop(0, cy, prepare, 0)

    def keep_mass(y, h, g, total):
        cr[DEEP + y, h, pl.ds(COARSE_PAD + 8 * g, 8), :] = 0.8 / (4.0 + total)
    coarse_sums(sums, keep_mass)

    pl.semaphore_wait(barrier, len(around))
    for copy in u_loads:
        copy.wait()
    for copy in f_loads:
        copy.wait()
    first_halos = send(("u0", ua, ua), ("f", f, f), ("r", r, r))
    start_along(first_halos, False)

    def region(src, dst, y0, y1, starts, load, rate):
        step = next(k for k in (2, 3, 1) if (y1 - y0) % k == 0)

        def body(i, carry):
            y = y0 + step * i
            for h in range(halves):
                for x in starts:
                    column = [at(src, y + j, h, x) for j in range(-1, step + 1)]
                    for j in range(step):
                        total = (column[j] + column[j + 2]) + (at(src, y + j, h, x - 1) + at(src, y + j, h, x + 1))
                        new = 0.2 * column[j + 1] + at(rate, y + j, h, x) * (at(load, y + j, h, x) + total)
                        dst[y + j, h, pl.ds(x, 8), :] = new
            return carry
        lax.fori_loop(0, (y1 - y0) // step, body, 0)

    def interior(src, dst, inset):
        region(src, dst, ROW_PAD + inset, ROW_PAD + ny - inset, windows(COL_PAD, nx, -inset), f, r)

    def frame(src, dst, inset, reach):
        full = windows(COL_PAD, nx, reach)
        region(src, dst, ROW_PAD - reach, ROW_PAD + inset, own, f, r)
        region(src, dst, ROW_PAD + ny - inset, ROW_PAD + ny + reach, own, f, r)
        region(src, dst, ROW_PAD, ROW_PAD + ny, [full[0], full[-1]], f, r)

    def defect(y0, y1, starts):
        def body(y, carry):
            for h in range(halves):
                for x in starts:
                    a, b, c, e = left_over(ua, f, d, ROW_PAD + RATIO * y, h, x)
                    sums[y, h, pl.ds(x - COL_PAD, 8), :] = (a + b) + (c + e)
            return carry
        lax.fori_loop(y0, y1, body, 0)

    interior(ua, ub, 1)
    interior(ub, uc, 2)
    start_along(first_halos, True)
    r3 = start(send(("r3", r, r)))
    arrived(first_halos)
    frame(ua, ub, 1, 1)
    frame(ub, uc, 2, 0)
    u2 = send(("u2", uc, uc))
    start_along(u2, False)
    gone(first_halos)

    interior(uc, ua, 1)
    defect(1, cy - 1, own[1:-1])
    start_along(u2, True)
    coarse_mass = start(send(("cr", cr, cr)))
    interior(ua, ud, 2)
    arrived(u2)
    frame(uc, ua, 1, 1)
    defect(0, 1, own)
    defect(cy - 1, cy, own)
    defect(1, cy - 1, [own[0], own[-1]])

    def keep_load(y, h, g, total):
        cl[DEEP + y, h, pl.ds(COARSE_PAD + 8 * g, 8), :] = total
    coarse_sums(sums, keep_load)
    coarse_load = send(("cl", cl, cl))
    start_along(coarse_load, False)
    frame(ua, ud, 2, 0)

    interior(ud, ub, 1)
    start_along(coarse_load, True)
    v4 = start(send(("v4", ud, ud)))
    interior(ub, ue, 2)

    arrived(coarse_mass)
    arrived(coarse_load)

    def first_coarse(y, carry):
        for h in range(halves):
            for x in windows(COARSE_PAD, cx, DEEP - 1):
                ca[y, h, pl.ds(x, 8), :] = at(cr, y, h, x) * at(cl, y, h, x)
        return carry
    lax.fori_loop(1, cy + 2 * DEEP - 1, first_coarse, 0)

    order = [ca, cb, ca, cb, cc, ca, cb, ca, cb]
    for k in range(1, INNER):
        reach = FIRST - 1 - k if k < FIRST else INNER - k
        if k == FIRST:
            coarse_values = start(send(("cv", cc, cc)))
            arrived(v4)
            frame(ud, ub, 1, 1)
            frame(ub, ue, 2, 0)
            v6 = start(send(("v6", ue, ue)))
            arrived(coarse_values)
        region(order[k - 1], order[k], DEEP - reach, DEEP + cy + reach, windows(COARSE_PAD, cx, reach), cl, cr)
    now = order[-1]

    def spread_row(y, carry):
        for h in range(halves):
            for w in range((cx + 2 + 7) // 8):
                c = at(now, DEEP - 1 + y, h, COARSE_PAD - 1 + 8 * w)
                for k in range(RATIO):
                    spread[y, h, pl.ds(32 * w + k, 8, stride=4), :] = c
        return carry
    lax.fori_loop(0, cy + 2, spread_row, 0)

    arrived(r3)
    gone(u2)

    def swept(y, rows, starts):
        for h in range(halves):
            for x in starts:
                e = x - COL_PAD + 4
                here = spread[y, h, pl.ds(e, 8), :]
                beside = spread[y, h, pl.ds(e - 1, 8), :] + spread[y, h, pl.ds(e + 1, 8), :]
                kept = 0.2 * here
                for j in rows:
                    if j == 0:
                        total = beside + (here + spread[y - 1, h, pl.ds(e, 8), :])
                    elif j == RATIO - 1:
                        total = beside + (here + spread[y + 1, h, pl.ds(e, 8), :])
                    else:
                        total = beside + (here + here)
                    uc[RATIO * y + j, h, pl.ds(x, 8), :] = kept + at(r, RATIO * y + j, h, x) * total

    reach3 = windows(COL_PAD, nx, 3)

    def first_swept(y, carry):
        swept(y, range(RATIO), reach3)
        return carry
    lax.fori_loop(1, cy + 1, first_swept, 0)
    swept(0, range(1, RATIO), reach3)
    swept(cy + 1, range(RATIO - 1), reach3)

    starts = windows(COL_PAD, nx, 2)

    def second_swept(i, carry):
        for h in range(halves):
            for x in starts:
                swept_twice(uc, r, None, ub, ROW_PAD - 2 + 2 * i, h, x)
        return carry
    lax.fori_loop(0, (ny + 4) // 2, second_swept, 0)
    arrived(v6)

    for made in (r3, coarse_mass, coarse_load, v4, coarse_values, v6):
        gone(made)


def local(n_row, n_col, source_terms, initial_values, absorption):
    ny, nx, layers = source_terms.shape
    halves = layers // LANES
    sizes = (ny, nx, halves, n_row, n_col)
    _, _, count = plan(ny, nx)
    fine = (ny + 2 * ROW_PAD, halves, nx + 2 * COL_PAD, LANES)
    block = (ny, halves, nx, LANES)
    cy, cx = ny // RATIO, nx // RATIO
    coarse = pltpu.VMEM((cy + 2 * DEEP, halves, cx + 2 * COARSE_PAD, LANES), jnp.float32)

    def vmem(shape):
        return pltpu.VMEM(shape, jnp.float32)

    anywhere = pl.BlockSpec(memory_space=pltpu.HBM)
    inside = pl.BlockSpec(memory_space=pltpu.VMEM)
    held = pl.pallas_call(
        functools.partial(kernel, sizes),
        out_shape=(vmem(fine), vmem(fine), vmem(fine), vmem(block), vmem(fine)),
        in_specs=[anywhere] * 3,
        out_specs=(inside,) * 5,
        scratch_shapes=[
            vmem(fine), vmem(fine), vmem(fine),
            vmem((cy, halves, nx, LANES)),
            vmem((cy + 2, halves, (cx + 8) * RATIO, LANES)),
            coarse, coarse, coarse, coarse, coarse,
            pltpu.SemaphoreType.DMA((3 * halves,)),
            pltpu.SemaphoreType.DMA((count,)),
            pltpu.SemaphoreType.DMA((count,)),
        ],
        compiler_params=pltpu.CompilerParams(
            collective_id=0, has_side_effects=True, vmem_limit_bytes=25_300_000
        ),
        name="two_grids",
    )(source_terms, initial_values, absorption)
    shape = jax.ShapeDtypeStruct(source_terms.shape, jnp.float32)
    return pl.pallas_call(
        functools.partial(finish, (ny, nx, halves)),
        out_shape=(shape, shape),
        in_specs=[inside] * 5,
        out_specs=(anywhere, anywhere),
        scratch_shapes=[vmem(fine), vmem(block), pltpu.SemaphoreType.DMA((8 * halves,))],
        compiler_params=pltpu.CompilerParams(vmem_limit_bytes=14_000_000),
        name="finish",
    )(*held)


def solution(mesh):
    n_row, n_col = mesh.shape["row"], mesh.shape["col"]
    spec = P("row", "col", None)
    return jax.shard_map(
        functools.partial(local, n_row, n_col),
        mesh=mesh, in_specs=(spec, spec, spec), out_specs=(spec, spec), check_vma=False,
    )
```

```python
import functools

import jax
import jax.numpy as jnp
from jax import lax
from jax.experimental import pallas as pl
from jax.experimental.pallas import tpu as pltpu
from jax.sharding import PartitionSpec as P

RATIO = 4
INNER = 9
LANES = 128
ROW_PAD = 4
COL_PAD = 8
FIRST = 5
DEEP = INNER - FIRST + 1
COARSE_PAD = 8
MESH = pl.DeviceIdType.MESH


def edge_rects(rows, cols, near, far):
    (y0, ny), (x0, nx) = rows, cols
    wide = far - near
    return [
        (0, 1, (y0, ny, x0 + nx - far, wide), (y0, ny, x0 - far, wide)),
        (0, -1, (y0, ny, x0 + near, wide), (y0, ny, x0 + nx + near, wide)),
        (1, 0, (y0 + ny - far, wide, x0, nx), (y0 - far, wide, x0, nx)),
        (-1, 0, (y0 + near, wide, x0, nx), (y0 + ny + near, wide, x0, nx)),
    ]


def corner_rects(rows, cols, near_y, far_y, far_x):
    (y0, ny), (x0, nx) = rows, cols
    wide = far_y - near_y
    found = []
    for dy in (1, -1):
        if dy == 1:
            from_y, to_y = y0 + ny - far_y, y0 - far_y
        else:
            from_y, to_y = y0 + near_y, y0 + ny + near_y
        for dx in (1, -1):
            if dx == 1:
                from_x, to_x = x0 + nx - far_x, x0 - far_x
            else:
                from_x, to_x = x0, x0 + nx
            found.append((dy, dx, (from_y, wide, from_x, far_x), (to_y, wide, to_x, far_x)))
    return found


def plan(ny, nx):
    rows, cols = (ROW_PAD, ny), (COL_PAD, nx)
    crows, ccols = (DEEP, ny // RATIO), (COARSE_PAD, nx // RATIO)
    coarse = edge_rects(crows, ccols, 0, DEEP - 1)
    coarse = coarse + corner_rects(crows, ccols, 0, 2, 4) + corner_rects(crows, ccols, 2, 4, 2)
    values = edge_rects(crows, ccols, 0, DEEP)
    values = values + corner_rects(crows, ccols, 0, 3, 5) + corner_rects(crows, ccols, 3, 5, 2)
    exchanges = {
        "u0": edge_rects(rows, cols, 0, 2) + corner_rects(rows, cols, 0, 1, 1),
        "f": edge_rects(rows, cols, 0, 1),
        "r": edge_rects(rows, cols, 0, 1),
        "r3": edge_rects(rows, cols, 1, 3) + corner_rects(rows, cols, 0, 2, 2),
        "u2": edge_rects(rows, cols, 0, 2) + corner_rects(rows, cols, 0, 1, 1),
        "cr": coarse,
        "cl": coarse,
        "v4": edge_rects(rows, cols, 0, 2) + corner_rects(rows, cols, 0, 1, 1),
        "v6": edge_rects(rows, cols, 0, 1),
        "cv": values,
    }
    at, first = 0, {}
    for name, rects in exchanges.items():
        first[name] = at
        at += len(rects)
    return exchanges, first, at


def left_over(u, f, d, y, h, x):
    column = [u[y + j, h, pl.ds(x, 8), :] for j in range(-1, RATIO + 1)]
    found = []
    for j in range(RATIO):
        beside = u[y + j, h, pl.ds(x - 1, 8), :] + u[y + j, h, pl.ds(x + 1, 8), :]
        total = f[y + j, h, pl.ds(x, 8), :] + ((column[j] + column[j + 2]) + beside)
        found.append(total - d[y + j - ROW_PAD, h, pl.ds(x - COL_PAD, 8), :] * column[j + 1])
    return found


def windows(x0, n, reach):
    low, high = x0 - reach, x0 + n + reach
    return [min(x, high - 8) for x in range(low, high, 8)]


def swept_twice(src, r, base, dst, y, h, x):
    column = [src[y + j, h, pl.ds(x, 8), :] for j in range(-1, 3)]
    for j in range(2):
        beside = src[y + j, h, pl.ds(x - 1, 8), :] + src[y + j, h, pl.ds(x + 1, 8), :]
        total = (column[j] + column[j + 2]) + beside
        new = 0.2 * column[j + 1] + r[y + j, h, pl.ds(x, 8), :] * total
        if base is not None:
            new = base[y + j, h, pl.ds(x, 8), :] + new
        dst[y + j, h, pl.ds(x, 8), :] = new


def finish(sizes, e, v, f, d, r, improved_hbm, remaining_hbm, u, left, store_sem):
    ny, nx, halves = sizes
    cy = ny // RATIO

    def stores(k, ref, hbm, y0, x0, y, rows):
        made = []
        for h in range(halves):
            made.append(pltpu.make_async_copy(
                ref.at[pl.ds(y0 + y, rows), h, pl.ds(x0, nx), :],
                hbm.at[pl.ds(y, rows), :, pl.ds(h * LANES, LANES)],
                store_sem.at[k * halves + h]))
        for copy in made:
            copy.start()
        return made

    going = []
    parts = 4
    starts = windows(COL_PAD, nx, 1)
    rows = ny // parts
    for part in range(parts):
        low = part * rows + 1 if part else -1

        def last(i, carry):
            for h in range(halves):
                for x in starts:
                    swept_twice(e, r, v, u, ROW_PAD + low + 2 * i, h, x)
            return carry
        lax.fori_loop(0, ((part + 1) * rows + 1 - low) // 2, last, 0)
        going += stores(2 * part, u, improved_hbm, ROW_PAD, COL_PAD, part * rows, rows)

        def remain(y, carry):
            for h in range(halves):
                for k in range(nx // 8):
                    for j, found in enumerate(left_over(u, f, d, ROW_PAD + RATIO * y, h, COL_PAD + 8 * k)):
                        left[RATIO * y + j, h, pl.ds(8 * k, 8), :] = found
            return carry
        lax.fori_loop(part * cy // parts, (part + 1) * cy // parts, remain, 0)
        going += stores(2 * part + 1, left, remaining_hbm, 0, 0, part * ny // parts, ny // parts)
    for copy in going:
        copy.wait()


def kernel(sizes, f_hbm, u_hbm, a_hbm, ub, ue, f, d, r,
           ua, uc, ud, sums, spread, cl, cr, ca, cb, cc,
           load_sem, send_sem, recv_sem):
    ny, nx, halves, n_row, n_col = sizes
    cy, cx = ny // RATIO, nx // RATIO
    exchanges, first, _ = plan(ny, nx)
    me_row, me_col = lax.axis_index("row"), lax.axis_index("col")

    def neighbour(dy, dx):
        return (lax.rem(me_row + dy + n_row, n_row), lax.rem(me_col + dx + n_col, n_col))

    def box(ref, where):
        y, h, x, w = where
        return ref.at[pl.ds(y, h), :, pl.ds(x, w), :]

    def copies(name, source, landing):
        made = []
        for k, (dy, dx, src, dst) in enumerate(exchanges[name]):
            made.append(pltpu.make_async_remote_copy(
                src_ref=box(source, src), dst_ref=box(landing, dst),
                send_sem=send_sem.at[first[name] + k], recv_sem=recv_sem.at[first[name] + k],
                device_id=neighbour(dy, dx), device_id_type=MESH))
        return made

    def send(*given):
        return [copies(*one) for one in given]

    def start(made):
        for part in made:
            for copy in part:
                copy.start()
        return made

    def gone(made):
        for part in made:
            for copy in part:
                copy.wait_send()

    def arrived(made):
        for part in made:
            for copy in part:
                copy.wait_recv()

    barrier = pltpu.get_barrier_semaphore()
    around = [(dy, dx) for dy in (-1, 0, 1) for dx in (-1, 0, 1) if (dy, dx) != (0, 0)]
    for dy, dx in around:
        pl.semaphore_signal(barrier, inc=1, device_id=neighbour(dy, dx), device_id_type=MESH)

    def loads(k, hbm, ref, y0, x0):
        made = []
        for h in range(halves):
            made.append(pltpu.make_async_copy(
                hbm.at[:, :, pl.ds(h * LANES, LANES)],
                ref.at[pl.ds(y0, ny), h, pl.ds(x0, nx), :],
                load_sem.at[k * halves + h]))
        for copy in made:
            copy.start()
        return made

    u_loads = loads(0, u_hbm, ua, ROW_PAD, COL_PAD)
    f_loads = loads(1, f_hbm, f, ROW_PAD, COL_PAD)
    a_loads = loads(2, a_hbm, d, 0, 0)

    pl.semaphore_wait(barrier, len(around))
    for copy in u_loads:
        copy.wait()
    first_halos = start(send(("u0", ua, ua)))
    for copy in f_loads:
        copy.wait()
    first_halos += start(send(("f", f, f)))

    own = [COL_PAD + 8 * k for k in range(nx // 8)]

    def at(ref, y, h, x):
        return ref[y, h, pl.ds(x, 8), :]

    def coarse_sums(ref, done):
        def body(y, carry):
            for h in range(halves):
                for g in range(cx // 8):
                    parts = [sums[y, h, pl.ds(32 * g + k, 8, stride=4), :] for k in range(4)]
                    total = ((parts[0] + parts[1]) + (parts[2] + parts[3])) * 0.25
                    done(y, h, g, total)
            return carry
        lax.fori_loop(0, cy, body, 0)

    for copy in a_loads:
        copy.wait()

    def prepare(y, carry):
        for h in range(halves):
            for k in range(nx // 8):
                total = None
                for j in range(RATIO):
                    a = d[RATIO * y + j, h, pl.ds(8 * k, 8), :]
                    here = 4.0 + a
                    d[RATIO * y + j, h, pl.ds(8 * k, 8), :] = here
                    r[ROW_PAD + RATIO * y + j, h, pl.ds(COL_PAD + 8 * k, 8), :] = 0.8 / here
                    total = a if total is None else total + a
                sums[y, h, pl.ds(8 * k, 8), :] = total
        return carry
    lax.fori_loop(0, cy, prepare, 0)
    first_halos += start(send(("r", r, r)))
    r3 = start(send(("r3", r, r)))

    def keep_mass(y, h, g, total):
        cr[DEEP + y, h, pl.ds(COARSE_PAD + 8 * g, 8), :] = 0.8 / (4.0 + total)
    coarse_sums(sums, keep_mass)

    def region(src, dst, y0, y1, starts, load, rate):
        step = next(k for k in (2, 3, 1) if (y1 - y0) % k == 0)

        def body(i, carry):
            y = y0 + step * i
            for h in range(halves):
                for x in starts:
                    column = [at(src, y + j, h, x) for j in range(-1, step + 1)]
                    for j in range(step):
                        total = (column[j] + column[j + 2]) + (at(src, y + j, h, x - 1) + at(src, y + j, h, x + 1))
                        new = 0.2 * column[j + 1] + at(rate, y + j, h, x) * (at(load, y + j, h, x) + total)
                        dst[y + j, h, pl.ds(x, 8), :] = new
            return carry
        lax.fori_loop(0, (y1 - y0) // step, body, 0)

    def interior(src, dst, inset):
        region(src, dst, ROW_PAD + inset, ROW_PAD + ny - inset, windows(COL_PAD, nx, -inset), f, r)

    def frame(src, dst, inset, reach):
        full = windows(COL_PAD, nx, reach)
        region(src, dst, ROW_PAD - reach, ROW_PAD + inset, own, f, r)
        region(src, dst, ROW_PAD + ny - inset, ROW_PAD + ny + reach, own, f, r)
        region(src, dst, ROW_PAD, ROW_PAD + ny, [full[0], full[-1]], f, r)

    def defect(y0, y1, starts):
        def body(y, carry):
            for h in range(halves):
                for x in starts:
                    a, b, c, e = left_over(ua, f, d, ROW_PAD + RATIO * y, h, x)
                    sums[y, h, pl.ds(x - COL_PAD, 8), :] = (a + b) + (c + e)
            return carry
        lax.fori_loop(y0, y1, body, 0)

    interior(ua, ub, 1)
    interior(ub, uc, 2)
    arrived(first_halos)
    frame(ua, ub, 1, 1)
    frame(ub, uc, 2, 0)
    u2 = start(send(("u2", uc, uc)))
    coarse_mass = start(send(("cr", cr, cr)))
    gone(first_halos)

    interior(uc, ua, 1)
    defect(1, cy - 1, own[1:-1])
    interior(ua, ud, 2)
    arrived(u2)
    frame(uc, ua, 1, 1)
    defect(0, 1, own)
    defect(cy - 1, cy, own)
    defect(1, cy - 1, [own[0], own[-1]])

    def keep_load(y, h, g, total):
        cl[DEEP + y, h, pl.ds(COARSE_PAD + 8 * g, 8), :] = total
    coarse_sums(sums, keep_load)
    coarse_load = start(send(("cl", cl, cl)))
    frame(ua, ud, 2, 0)
    v4 = start(send(("v4", ud, ud)))

    interior(ud, ub, 1)
    interior(ub, ue, 2)

    arrived(coarse_mass)
    arrived(coarse_load)

    def first_coarse(y, carry):
        for h in range(halves):
            for x in windows(COARSE_PAD, cx, DEEP - 1):
                ca[y, h, pl.ds(x, 8), :] = at(cr, y, h, x) * at(cl, y, h, x)
        return carry
    lax.fori_loop(1, cy + 2 * DEEP - 1, first_coarse, 0)

    order = [ca, cb, ca, cb, cc, ca, cb, ca, cb]
    for k in range(1, INNER):
        reach = FIRST - 1 - k if k < FIRST else INNER - k
        if k == FIRST:
            coarse_values = start(send(("cv", cc, cc)))
            arrived(v4)
            frame(ud, ub, 1, 1)
            frame(ub, ue, 2, 0)
            v6 = start(send(("v6", ue, ue)))
            arrived(coarse_values)
        region(order[k - 1], order[k], DEEP - reach, DEEP + cy + reach, windows(COARSE_PAD, cx, reach), cl, cr)
    now = order[-1]

    def spread_row(y, carry):
        for h in range(halves):
            for w in range((cx + 2 + 7) // 8):
                c = at(now, DEEP - 1 + y, h, COARSE_PAD - 1 + 8 * w)
                for k in range(RATIO):
                    spread[y, h, pl.ds(32 * w + k, 8, stride=4), :] = c
        return carry
    lax.fori_loop(0, cy + 2, spread_row, 0)

    arrived(r3)
    gone(u2)

    def swept(y, rows, starts):
        for h in range(halves):
            for x in starts:
                e = x - COL_PAD + 4
                here = spread[y, h, pl.ds(e, 8), :]
                beside = spread[y, h, pl.ds(e - 1, 8), :] + spread[y, h, pl.ds(e + 1, 8), :]
                kept = 0.2 * here
                for j in rows:
                    if j == 0:
                        total = beside + (here + spread[y - 1, h, pl.ds(e, 8), :])
                    elif j == RATIO - 1:
                        total = beside + (here + spread[y + 1, h, pl.ds(e, 8), :])
                    else:
                        total = beside + (here + here)
                    uc[RATIO * y + j, h, pl.ds(x, 8), :] = kept + at(r, RATIO * y + j, h, x) * total

    reach3 = windows(COL_PAD, nx, 3)

    def first_swept(y, carry):
        swept(y, range(RATIO), reach3)
        return carry
    lax.fori_loop(1, cy + 1, first_swept, 0)
    swept(0, range(1, RATIO), reach3)
    swept(cy + 1, range(RATIO - 1), reach3)

    starts = windows(COL_PAD, nx, 2)

    def second_swept(i, carry):
        for h in range(halves):
            for x in starts:
                swept_twice(uc, r, None, ub, ROW_PAD - 2 + 2 * i, h, x)
        return carry
    lax.fori_loop(0, (ny + 4) // 2, second_swept, 0)
    arrived(v6)

    for made in (r3, coarse_mass, coarse_load, v4, coarse_values, v6):
        gone(made)


def local(n_row, n_col, source_terms, initial_values, absorption):
    ny, nx, layers = source_terms.shape
    halves = layers // LANES
    sizes = (ny, nx, halves, n_row, n_col)
    _, _, count = plan(ny, nx)
    fine = (ny + 2 * ROW_PAD, halves, nx + 2 * COL_PAD, LANES)
    block = (ny, halves, nx, LANES)
    cy, cx = ny // RATIO, nx // RATIO
    coarse = pltpu.VMEM((cy + 2 * DEEP, halves, cx + 2 * COARSE_PAD, LANES), jnp.float32)

    def vmem(shape):
        return pltpu.VMEM(shape, jnp.float32)

    anywhere = pl.BlockSpec(memory_space=pltpu.HBM)
    inside = pl.BlockSpec(memory_space=pltpu.VMEM)
    held = pl.pallas_call(
        functools.partial(kernel, sizes),
        out_shape=(vmem(fine), vmem(fine), vmem(fine), vmem(block), vmem(fine)),
        in_specs=[anywhere] * 3,
        out_specs=(inside,) * 5,
        scratch_shapes=[
            vmem(fine), vmem(fine), vmem(fine),
            vmem((cy, halves, nx, LANES)),
            vmem((cy + 2, halves, (cx + 8) * RATIO, LANES)),
            coarse, coarse, coarse, coarse, coarse,
            pltpu.SemaphoreType.DMA((3 * halves,)),
            pltpu.SemaphoreType.DMA((count,)),
            pltpu.SemaphoreType.DMA((count,)),
        ],
        compiler_params=pltpu.CompilerParams(
            collective_id=0, has_side_effects=True, vmem_limit_bytes=25_300_000
        ),
        name="two_grids",
    )(source_terms, initial_values, absorption)
    shape = jax.ShapeDtypeStruct(source_terms.shape, jnp.float32)
    return pl.pallas_call(
        functools.partial(finish, (ny, nx, halves)),
        out_shape=(shape, shape),
        in_specs=[inside] * 5,
        out_specs=(anywhere, anywhere),
        scratch_shapes=[vmem(fine), vmem(block), pltpu.SemaphoreType.DMA((8 * halves,))],
        compiler_params=pltpu.CompilerParams(vmem_limit_bytes=14_000_000),
        name="finish",
    )(*held)


def solution(mesh):
    n_row, n_col = mesh.shape["row"], mesh.shape["col"]
    spec = P("row", "col", None)
    return jax.shard_map(
        functools.partial(local, n_row, n_col),
        mesh=mesh, in_specs=(spec, spec, spec), out_specs=(spec, spec), check_vma=False,
    )
```

```python
import functools

import jax
import jax.numpy as jnp
from jax import lax
from jax.experimental import pallas as pl
from jax.experimental.pallas import tpu as pltpu
from jax.sharding import PartitionSpec as P

RATIO = 4
INNER = 9
LANES = 128
ROW_PAD = 4
COL_PAD = 8
FIRST = 5
DEEP = INNER - FIRST + 1
COARSE_PAD = 8
MESH = pl.DeviceIdType.MESH


def edge_rects(rows, cols, near, far):
    (y0, ny), (x0, nx) = rows, cols
    wide = far - near
    return [
        (0, 1, (y0, ny, x0 + nx - far, wide), (y0, ny, x0 - far, wide)),
        (0, -1, (y0, ny, x0 + near, wide), (y0, ny, x0 + nx + near, wide)),
        (1, 0, (y0 + ny - far, wide, x0, nx), (y0 - far, wide, x0, nx)),
        (-1, 0, (y0 + near, wide, x0, nx), (y0 + ny + near, wide, x0, nx)),
    ]


def corner_rects(rows, cols, near_y, far_y, far_x):
    (y0, ny), (x0, nx) = rows, cols
    wide = far_y - near_y
    found = []
    for dy in (1, -1):
        if dy == 1:
            from_y, to_y = y0 + ny - far_y, y0 - far_y
        else:
            from_y, to_y = y0 + near_y, y0 + ny + near_y
        for dx in (1, -1):
            if dx == 1:
                from_x, to_x = x0 + nx - far_x, x0 - far_x
            else:
                from_x, to_x = x0, x0 + nx
            found.append((dy, dx, (from_y, wide, from_x, far_x), (to_y, wide, to_x, far_x)))
    return found


def plan(ny, nx):
    rows, cols = (ROW_PAD, ny), (COL_PAD, nx)
    crows, ccols = (DEEP, ny // RATIO), (COARSE_PAD, nx // RATIO)
    coarse = edge_rects(crows, ccols, 0, DEEP - 1)
    coarse = coarse + corner_rects(crows, ccols, 0, 2, 4) + corner_rects(crows, ccols, 2, 4, 2)
    values = edge_rects(crows, ccols, 0, DEEP)
    values = values + corner_rects(crows, ccols, 0, 3, 5) + corner_rects(crows, ccols, 3, 5, 2)
    exchanges = {
        "u0": edge_rects(rows, cols, 0, 2) + corner_rects(rows, cols, 0, 1, 1),
        "f": edge_rects(rows, cols, 0, 1),
        "r": edge_rects(rows, cols, 0, 1),
        "r3": edge_rects(rows, cols, 1, 3) + corner_rects(rows, cols, 0, 2, 2),
        "u2": edge_rects(rows, cols, 0, 2) + corner_rects(rows, cols, 0, 1, 1),
        "cr": coarse,
        "cl": coarse,
        "v4": edge_rects(rows, cols, 0, 2) + corner_rects(rows, cols, 0, 1, 1),
        "v6": edge_rects(rows, cols, 0, 1),
        "cv": values,
    }
    at, first = 0, {}
    for name, rects in exchanges.items():
        first[name] = at
        at += len(rects)
    return exchanges, first, at


def left_over(u, f, d, y, h, x):
    column = [u[y + j, h, pl.ds(x, 8), :] for j in range(-1, RATIO + 1)]
    found = []
    for j in range(RATIO):
        beside = u[y + j, h, pl.ds(x - 1, 8), :] + u[y + j, h, pl.ds(x + 1, 8), :]
        total = f[y + j, h, pl.ds(x, 8), :] + ((column[j] + column[j + 2]) + beside)
        found.append(total - d[y + j - ROW_PAD, h, pl.ds(x - COL_PAD, 8), :] * column[j + 1])
    return found


def windows(x0, n, reach):
    low, high = x0 - reach, x0 + n + reach
    return [min(x, high - 8) for x in range(low, high, 8)]


def loop(low, high, times, one):
    times = times if (high - low) % times == 0 else 1

    def body(i, carry):
        for t in range(times):
            one(low + i * times + t)
        return carry
    lax.fori_loop(0, (high - low) // times, body, 0)


def swept_twice(src, r, base, dst, y, h, x):
    column = [src[y + j, h, pl.ds(x, 8), :] for j in range(-1, 3)]
    for j in range(2):
        beside = src[y + j, h, pl.ds(x - 1, 8), :] + src[y + j, h, pl.ds(x + 1, 8), :]
        total = (column[j] + column[j + 2]) + beside
        new = 0.2 * column[j + 1] + r[y + j, h, pl.ds(x, 8), :] * total
        if base is not None:
            new = base[y + j, h, pl.ds(x, 8), :] + new
        dst[y + j, h, pl.ds(x, 8), :] = new


def finish(sizes, e, v, f, d, r, improved_hbm, remaining_hbm, u, left, store_sem):
    ny, nx, halves = sizes
    cy = ny // RATIO

    def stores(k, ref, hbm, y0, x0, y, rows):
        made = []
        for h in range(halves):
            made.append(pltpu.make_async_copy(
                ref.at[pl.ds(y0 + y, rows), h, pl.ds(x0, nx), :],
                hbm.at[pl.ds(y, rows), :, pl.ds(h * LANES, LANES)],
                store_sem.at[k * halves + h]))
        for copy in made:
            copy.start()
        return made

    going = []
    parts = 4
    starts = windows(COL_PAD, nx, 1)
    rows = ny // parts
    for part in range(parts):
        low = part * rows + 1 if part else -1

        def last(i, carry):
            for h in range(halves):
                for x in starts:
                    swept_twice(e, r, v, u, ROW_PAD + low + 2 * i, h, x)
            return carry
        lax.fori_loop(0, ((part + 1) * rows + 1 - low) // 2, last, 0)
        going += stores(2 * part, u, improved_hbm, ROW_PAD, COL_PAD, part * rows, rows)

        def remain(y, carry):
            for h in range(halves):
                for k in range(nx // 8):
                    for j, found in enumerate(left_over(u, f, d, ROW_PAD + RATIO * y, h, COL_PAD + 8 * k)):
                        left[RATIO * y + j, h, pl.ds(8 * k, 8), :] = found
            return carry
        lax.fori_loop(part * cy // parts, (part + 1) * cy // parts, remain, 0)
        going += stores(2 * part + 1, left, remaining_hbm, 0, 0, part * ny // parts, ny // parts)
    for copy in going:
        copy.wait()


def kernel(sizes, f_hbm, u_hbm, a_hbm, ub, ue, f, d, r,
           ua, uc, ud, sums, spread, cl, cr, ca, cb, cc,
           load_sem, send_sem, recv_sem):
    ny, nx, halves, n_row, n_col = sizes
    cy, cx = ny // RATIO, nx // RATIO
    exchanges, first, _ = plan(ny, nx)
    me_row, me_col = lax.axis_index("row"), lax.axis_index("col")

    def neighbour(dy, dx):
        return (lax.rem(me_row + dy + n_row, n_row), lax.rem(me_col + dx + n_col, n_col))

    def box(ref, where):
        y, h, x, w = where
        return ref.at[pl.ds(y, h), :, pl.ds(x, w), :]

    def copies(name, source, landing):
        made = []
        for k, (dy, dx, src, dst) in enumerate(exchanges[name]):
            made.append(pltpu.make_async_remote_copy(
                src_ref=box(source, src), dst_ref=box(landing, dst),
                send_sem=send_sem.at[first[name] + k], recv_sem=recv_sem.at[first[name] + k],
                device_id=neighbour(dy, dx), device_id_type=MESH))
        return made

    def send(*given):
        return [copies(*one) for one in given]

    def start(made):
        for part in made:
            for copy in part:
                copy.start()
        return made

    def gone(made):
        for part in made:
            for copy in part:
                copy.wait_send()

    def arrived(made):
        for part in made:
            for copy in part:
                copy.wait_recv()

    barrier = pltpu.get_barrier_semaphore()
    around = [(dy, dx) for dy in (-1, 0, 1) for dx in (-1, 0, 1) if (dy, dx) != (0, 0)]
    for dy, dx in around:
        pl.semaphore_signal(barrier, inc=1, device_id=neighbour(dy, dx), device_id_type=MESH)

    def loads(k, hbm, ref, y0, x0):
        made = []
        for h in range(halves):
            made.append(pltpu.make_async_copy(
                hbm.at[:, :, pl.ds(h * LANES, LANES)],
                ref.at[pl.ds(y0, ny), h, pl.ds(x0, nx), :],
                load_sem.at[k * halves + h]))
        for copy in made:
            copy.start()
        return made

    u_loads = loads(0, u_hbm, ua, ROW_PAD, COL_PAD)
    f_loads = loads(1, f_hbm, f, ROW_PAD, COL_PAD)
    a_loads = loads(2, a_hbm, d, 0, 0)

    pl.semaphore_wait(barrier, len(around))
    for copy in u_loads:
        copy.wait()
    first_halos = start(send(("u0", ua, ua)))
    for copy in f_loads:
        copy.wait()
    first_halos += start(send(("f", f, f)))

    own = [COL_PAD + 8 * k for k in range(nx // 8)]

    def at(ref, y, h, x):
        return ref[y, h, pl.ds(x, 8), :]

    def coarse_sums(ref, done):
        def one(y):
            for h in range(halves):
                for g in range(cx // 8):
                    parts = [sums[y, h, pl.ds(32 * g + k, 8, stride=4), :] for k in range(4)]
                    total = ((parts[0] + parts[1]) + (parts[2] + parts[3])) * 0.25
                    done(y, h, g, total)
        loop(0, cy, 4, one)

    for copy in a_loads:
        copy.wait()

    def prepare(y, carry):
        for h in range(halves):
            for k in range(nx // 8):
                total = None
                for j in range(RATIO):
                    a = d[RATIO * y + j, h, pl.ds(8 * k, 8), :]
                    here = 4.0 + a
                    d[RATIO * y + j, h, pl.ds(8 * k, 8), :] = here
                    r[ROW_PAD + RATIO * y + j, h, pl.ds(COL_PAD + 8 * k, 8), :] = 0.8 / here
                    total = a if total is None else total + a
                sums[y, h, pl.ds(8 * k, 8), :] = total
        return carry
    lax.fori_loop(0, cy, prepare, 0)
    first_halos += start(send(("r", r, r)))
    r3 = start(send(("r3", r, r)))

    def keep_mass(y, h, g, total):
        cr[DEEP + y, h, pl.ds(COARSE_PAD + 8 * g, 8), :] = 0.8 / (4.0 + total)
    coarse_sums(sums, keep_mass)

    def region(src, dst, y0, y1, starts, load, rate):
        step = next(k for k in (8, 6, 4, 3, 2, 1) if (y1 - y0) % k == 0 and k * len(starts) <= 18)

        def body(i, carry):
            y = y0 + step * i
            for h in range(halves):
                for x in starts:
                    column = [at(src, y + j, h, x) for j in range(-1, step + 1)]
                    for j in range(step):
                        total = (column[j] + column[j + 2]) + (at(src, y + j, h, x - 1) + at(src, y + j, h, x + 1))
                        new = 0.2 * column[j + 1] + at(rate, y + j, h, x) * (at(load, y + j, h, x) + total)
                        dst[y + j, h, pl.ds(x, 8), :] = new
            return carry
        lax.fori_loop(0, (y1 - y0) // step, body, 0)

    def interior(src, dst, inset):
        region(src, dst, ROW_PAD + inset, ROW_PAD + ny - inset, windows(COL_PAD, nx, -inset), f, r)

    def frame(src, dst, inset, reach):
        full = windows(COL_PAD, nx, reach)
        region(src, dst, ROW_PAD - reach, ROW_PAD + inset, own, f, r)
        region(src, dst, ROW_PAD + ny - inset, ROW_PAD + ny + reach, own, f, r)
        region(src, dst, ROW_PAD, ROW_PAD + ny, [full[0], full[-1]], f, r)

    def defect(y0, y1, starts):
        def one(y):
            for h in range(halves):
                for x in starts:
                    a, b, c, e = left_over(ua, f, d, ROW_PAD + RATIO * y, h, x)
                    sums[y, h, pl.ds(x - COL_PAD, 8), :] = (a + b) + (c + e)
        loop(y0, y1, 2 if len(starts) <= 2 else 1, one)

    interior(ua, ub, 1)
    interior(ub, uc, 2)
    arrived(first_halos)
    frame(ua, ub, 1, 1)
    frame(ub, uc, 2, 0)
    u2 = start(send(("u2", uc, uc)))
    coarse_mass = start(send(("cr", cr, cr)))
    gone(first_halos)

    interior(uc, ua, 1)
    defect(1, cy - 1, own[1:-1])
    interior(ua, ud, 2)
    arrived(u2)
    frame(uc, ua, 1, 1)
    defect(0, 1, own)
    defect(cy - 1, cy, own)
    defect(1, cy - 1, [own[0], own[-1]])

    def keep_load(y, h, g, total):
        cl[DEEP + y, h, pl.ds(COARSE_PAD + 8 * g, 8), :] = total
    coarse_sums(sums, keep_load)
    coarse_load = start(send(("cl", cl, cl)))
    frame(ua, ud, 2, 0)
    v4 = start(send(("v4", ud, ud)))

    interior(ud, ub, 1)
    interior(ub, ue, 2)

    arrived(coarse_mass)
    arrived(coarse_load)

    def first_coarse(y):
        for h in range(halves):
            for x in windows(COARSE_PAD, cx, DEEP - 1):
                ca[y, h, pl.ds(x, 8), :] = at(cr, y, h, x) * at(cl, y, h, x)
    loop(1, cy + 2 * DEEP - 1, 4, first_coarse)

    order = [ca, cb, ca, cb, cc, ca, cb, ca, cb]
    for k in range(1, INNER):
        reach = FIRST - 1 - k if k < FIRST else INNER - k
        if k == FIRST:
            coarse_values = start(send(("cv", cc, cc)))
            arrived(v4)
            frame(ud, ub, 1, 1)
            frame(ub, ue, 2, 0)
            v6 = start(send(("v6", ue, ue)))
            arrived(coarse_values)
        region(order[k - 1], order[k], DEEP - reach, DEEP + cy + reach, windows(COARSE_PAD, cx, reach), cl, cr)
    now = order[-1]

    def spread_row(y):
        for h in range(halves):
            for w in range((cx + 2 + 7) // 8):
                c = at(now, DEEP - 1 + y, h, COARSE_PAD - 1 + 8 * w)
                for k in range(RATIO):
                    spread[y, h, pl.ds(32 * w + k, 8, stride=4), :] = c
    loop(0, cy + 2, 3, spread_row)

    arrived(r3)
    gone(u2)

    def swept(y, rows, starts):
        for h in range(halves):
            for x in starts:
                e = x - COL_PAD + 4
                here = spread[y, h, pl.ds(e, 8), :]
                beside = spread[y, h, pl.ds(e - 1, 8), :] + spread[y, h, pl.ds(e + 1, 8), :]
                kept = 0.2 * here
                for j in rows:
                    if j == 0:
                        total = beside + (here + spread[y - 1, h, pl.ds(e, 8), :])
                    elif j == RATIO - 1:
                        total = beside + (here + spread[y + 1, h, pl.ds(e, 8), :])
                    else:
                        total = beside + (here + here)
                    uc[RATIO * y + j, h, pl.ds(x, 8), :] = kept + at(r, RATIO * y + j, h, x) * total

    reach3 = windows(COL_PAD, nx, 3)

    def first_swept(y, carry):
        swept(y, range(RATIO), reach3)
        return carry
    lax.fori_loop(1, cy + 1, first_swept, 0)
    swept(0, range(1, RATIO), reach3)
    swept(cy + 1, range(RATIO - 1), reach3)

    starts = windows(COL_PAD, nx, 2)

    def second_swept(i, carry):
        for h in range(halves):
            for x in starts:
                swept_twice(uc, r, None, ub, ROW_PAD - 2 + 2 * i, h, x)
        return carry
    lax.fori_loop(0, (ny + 4) // 2, second_swept, 0)
    arrived(v6)

    for made in (r3, coarse_mass, coarse_load, v4, coarse_values, v6):
        gone(made)


def local(n_row, n_col, source_terms, initial_values, absorption):
    ny, nx, layers = source_terms.shape
    halves = layers // LANES
    sizes = (ny, nx, halves, n_row, n_col)
    _, _, count = plan(ny, nx)
    fine = (ny + 2 * ROW_PAD, halves, nx + 2 * COL_PAD, LANES)
    block = (ny, halves, nx, LANES)
    cy, cx = ny // RATIO, nx // RATIO
    coarse = pltpu.VMEM((cy + 2 * DEEP, halves, cx + 2 * COARSE_PAD, LANES), jnp.float32)

    def vmem(shape):
        return pltpu.VMEM(shape, jnp.float32)

    anywhere = pl.BlockSpec(memory_space=pltpu.HBM)
    inside = pl.BlockSpec(memory_space=pltpu.VMEM)
    held = pl.pallas_call(
        functools.partial(kernel, sizes),
        out_shape=(vmem(fine), vmem(fine), vmem(fine), vmem(block), vmem(fine)),
        in_specs=[anywhere] * 3,
        out_specs=(inside,) * 5,
        scratch_shapes=[
            vmem(fine), vmem(fine), vmem(fine),
            vmem((cy, halves, nx, LANES)),
            vmem((cy + 2, halves, (cx + 8) * RATIO, LANES)),
            coarse, coarse, coarse, coarse, coarse,
            pltpu.SemaphoreType.DMA((3 * halves,)),
            pltpu.SemaphoreType.DMA((count,)),
            pltpu.SemaphoreType.DMA((count,)),
        ],
        compiler_params=pltpu.CompilerParams(
            collective_id=0, has_side_effects=True, vmem_limit_bytes=25_300_000
        ),
        name="two_grids",
    )(source_terms, initial_values, absorption)
    shape = jax.ShapeDtypeStruct(source_terms.shape, jnp.float32)
    return pl.pallas_call(
        functools.partial(finish, (ny, nx, halves)),
        out_shape=(shape, shape),
        in_specs=[inside] * 5,
        out_specs=(anywhere, anywhere),
        scratch_shapes=[vmem(fine), vmem(block), pltpu.SemaphoreType.DMA((8 * halves,))],
        compiler_params=pltpu.CompilerParams(vmem_limit_bytes=14_000_000),
        name="finish",
    )(*held)


def solution(mesh):
    n_row, n_col = mesh.shape["row"], mesh.shape["col"]
    spec = P("row", "col", None)
    return jax.shard_map(
        functools.partial(local, n_row, n_col),
        mesh=mesh, in_specs=(spec, spec, spec), out_specs=(spec, spec), check_vma=False,
    )
```

```python
import functools

import jax
import jax.numpy as jnp
from jax import lax
from jax.experimental import pallas as pl
from jax.experimental.pallas import tpu as pltpu
from jax.sharding import PartitionSpec as P

RATIO = 4
INNER = 9
LANES = 128
ROW_PAD = 4
COL_PAD = 8
FIRST = 5
DEEP = INNER - FIRST + 1
COARSE_PAD = 8
MESH = pl.DeviceIdType.MESH


def edge_rects(rows, cols, near, far):
    (y0, ny), (x0, nx) = rows, cols
    wide = far - near
    return [
        (0, 1, (y0, ny, x0 + nx - far, wide), (y0, ny, x0 - far, wide)),
        (0, -1, (y0, ny, x0 + near, wide), (y0, ny, x0 + nx + near, wide)),
        (1, 0, (y0 + ny - far, wide, x0, nx), (y0 - far, wide, x0, nx)),
        (-1, 0, (y0 + near, wide, x0, nx), (y0 + ny + near, wide, x0, nx)),
    ]


def corner_rects(rows, cols, near_y, far_y, far_x):
    (y0, ny), (x0, nx) = rows, cols
    wide = far_y - near_y
    found = []
    for dy in (1, -1):
        if dy == 1:
            from_y, to_y = y0 + ny - far_y, y0 - far_y
        else:
            from_y, to_y = y0 + near_y, y0 + ny + near_y
        for dx in (1, -1):
            if dx == 1:
                from_x, to_x = x0 + nx - far_x, x0 - far_x
            else:
                from_x, to_x = x0, x0 + nx
            found.append((dy, dx, (from_y, wide, from_x, far_x), (to_y, wide, to_x, far_x)))
    return found


def plan(ny, nx):
    rows, cols = (ROW_PAD, ny), (COL_PAD, nx)
    crows, ccols = (DEEP, ny // RATIO), (COARSE_PAD, nx // RATIO)
    coarse = corner_rects(crows, ccols, 0, 2, 4) + corner_rects(crows, ccols, 2, 4, 2)
    coarse = coarse + edge_rects(crows, ccols, 0, DEEP - 1)
    values = corner_rects(crows, ccols, 0, 3, 5) + corner_rects(crows, ccols, 3, 5, 2)
    values = values + edge_rects(crows, ccols, 0, DEEP)
    exchanges = {
        "u0": corner_rects(rows, cols, 0, 1, 1) + edge_rects(rows, cols, 0, 2),
        "f": edge_rects(rows, cols, 0, 1),
        "r": edge_rects(rows, cols, 0, 1),
        "r3": edge_rects(rows, cols, 1, 3) + corner_rects(rows, cols, 0, 2, 2),
        "u2": corner_rects(rows, cols, 0, 1, 1) + edge_rects(rows, cols, 0, 2),
        "cr": coarse,
        "cl": coarse,
        "v4": corner_rects(rows, cols, 0, 1, 1) + edge_rects(rows, cols, 0, 2),
        "v6": edge_rects(rows, cols, 0, 1),
        "cv": values,
    }
    at, first = 0, {}
    for name, rects in exchanges.items():
        first[name] = at
        at += len(rects)
    return exchanges, first, at


def left_over(u, f, d, y, h, x):
    column = [u[y + j, h, pl.ds(x, 8), :] for j in range(-1, RATIO + 1)]
    found = []
    for j in range(RATIO):
        beside = u[y + j, h, pl.ds(x - 1, 8), :] + u[y + j, h, pl.ds(x + 1, 8), :]
        total = f[y + j, h, pl.ds(x, 8), :] + ((column[j] + column[j + 2]) + beside)
        found.append(total - d[y + j - ROW_PAD, h, pl.ds(x - COL_PAD, 8), :] * column[j + 1])
    return found


def windows(x0, n, reach):
    low, high = x0 - reach, x0 + n + reach
    return [min(x, high - 8) for x in range(low, high, 8)]


def loop(low, high, times, one):
    times = times if (high - low) % times == 0 else 1

    def body(i, carry):
        for t in range(times):
            one(low + i * times + t)
        return carry
    lax.fori_loop(0, (high - low) // times, body, 0)


def swept_twice(src, r, base, dst, y, h, x):
    column = [src[y + j, h, pl.ds(x, 8), :] for j in range(-1, 3)]
    for j in range(2):
        beside = src[y + j, h, pl.ds(x - 1, 8), :] + src[y + j, h, pl.ds(x + 1, 8), :]
        total = (column[j] + column[j + 2]) + beside
        new = 0.2 * column[j + 1] + r[y + j, h, pl.ds(x, 8), :] * total
        if base is not None:
            new = base[y + j, h, pl.ds(x, 8), :] + new
        dst[y + j, h, pl.ds(x, 8), :] = new


def finish(sizes, e, v, f, d, r, improved_hbm, remaining_hbm, u, left, store_sem):
    ny, nx, halves = sizes
    cy = ny // RATIO

    def stores(k, ref, hbm, y0, x0, y, rows):
        made = []
        for h in range(halves):
            made.append(pltpu.make_async_copy(
                ref.at[pl.ds(y0 + y, rows), h, pl.ds(x0, nx), :],
                hbm.at[pl.ds(y, rows), :, pl.ds(h * LANES, LANES)],
                store_sem.at[k * halves + h]))
        for copy in made:
            copy.start()
        return made

    going = []
    parts = 4
    starts = windows(COL_PAD, nx, 1)
    rows = ny // parts
    for part in range(parts):
        low = part * rows + 1 if part else -1

        def last(i, carry):
            for h in range(halves):
                for x in starts:
                    swept_twice(e, r, v, u, ROW_PAD + low + 2 * i, h, x)
            return carry
        lax.fori_loop(0, ((part + 1) * rows + 1 - low) // 2, last, 0)
        going += stores(2 * part, u, improved_hbm, ROW_PAD, COL_PAD, part * rows, rows)

        def remain(y, carry):
            for h in range(halves):
                for k in range(nx // 8):
                    for j, found in enumerate(left_over(u, f, d, ROW_PAD + RATIO * y, h, COL_PAD + 8 * k)):
                        left[RATIO * y + j, h, pl.ds(8 * k, 8), :] = found
            return carry
        lax.fori_loop(part * cy // parts, (part + 1) * cy // parts, remain, 0)
        going += stores(2 * part + 1, left, remaining_hbm, 0, 0, part * ny // parts, ny // parts)
    for copy in going:
        copy.wait()


def kernel(sizes, f_hbm, u_hbm, a_hbm, ub, ue, f, d, r,
           ua, uc, ud, sums, spread, cl, cr, ca, cb, cc,
           load_sem, send_sem, recv_sem):
    ny, nx, halves, n_row, n_col = sizes
    cy, cx = ny // RATIO, nx // RATIO
    exchanges, first, _ = plan(ny, nx)
    me_row, me_col = lax.axis_index("row"), lax.axis_index("col")

    def neighbour(dy, dx):
        return (lax.rem(me_row + dy + n_row, n_row), lax.rem(me_col + dx + n_col, n_col))

    def box(ref, where):
        y, h, x, w = where
        return ref.at[pl.ds(y, h), :, pl.ds(x, w), :]

    def copies(name, source, landing):
        made = []
        for k, (dy, dx, src, dst) in enumerate(exchanges[name]):
            made.append(pltpu.make_async_remote_copy(
                src_ref=box(source, src), dst_ref=box(landing, dst),
                send_sem=send_sem.at[first[name] + k], recv_sem=recv_sem.at[first[name] + k],
                device_id=neighbour(dy, dx), device_id_type=MESH))
        return made

    def send(*given):
        return [copies(*one) for one in given]

    def start(made):
        for part in made:
            for copy in part:
                copy.start()
        return made

    def gone(made):
        for part in made:
            for copy in part:
                copy.wait_send()

    def arrived(made):
        for part in made:
            for copy in part:
                copy.wait_recv()

    barrier = pltpu.get_barrier_semaphore()
    around = [(dy, dx) for dy in (-1, 0, 1) for dx in (-1, 0, 1) if (dy, dx) != (0, 0)]
    for dy, dx in around:
        pl.semaphore_signal(barrier, inc=1, device_id=neighbour(dy, dx), device_id_type=MESH)

    def loads(k, hbm, ref, y0, x0):
        made = []
        for h in range(halves):
            made.append(pltpu.make_async_copy(
                hbm.at[:, :, pl.ds(h * LANES, LANES)],
                ref.at[pl.ds(y0, ny), h, pl.ds(x0, nx), :],
                load_sem.at[k * halves + h]))
        for copy in made:
            copy.start()
        return made

    u_loads = loads(0, u_hbm, ua, ROW_PAD, COL_PAD)
    f_loads = loads(1, f_hbm, f, ROW_PAD, COL_PAD)
    a_loads = loads(2, a_hbm, d, 0, 0)

    pl.semaphore_wait(barrier, len(around))
    for copy in u_loads:
        copy.wait()
    first_halos = start(send(("u0", ua, ua)))
    for copy in f_loads:
        copy.wait()
    first_halos += start(send(("f", f, f)))

    own = [COL_PAD + 8 * k for k in range(nx // 8)]

    def at(ref, y, h, x):
        return ref[y, h, pl.ds(x, 8), :]

    def coarse_sums(ref, done):
        def one(y):
            for h in range(halves):
                for g in range(cx // 8):
                    parts = [sums[y, h, pl.ds(32 * g + k, 8, stride=4), :] for k in range(4)]
                    total = ((parts[0] + parts[1]) + (parts[2] + parts[3])) * 0.25
                    done(y, h, g, total)
        loop(0, cy, 4, one)

    for copy in a_loads:
        copy.wait()

    def prepare(y, carry):
        for h in range(halves):
            for k in range(nx // 8):
                total = None
                for j in range(RATIO):
                    a = d[RATIO * y + j, h, pl.ds(8 * k, 8), :]
                    here = 4.0 + a
                    d[RATIO * y + j, h, pl.ds(8 * k, 8), :] = here
                    r[ROW_PAD + RATIO * y + j, h, pl.ds(COL_PAD + 8 * k, 8), :] = 0.8 / here
                    total = a if total is None else total + a
                sums[y, h, pl.ds(8 * k, 8), :] = total
        return carry
    lax.fori_loop(0, cy, prepare, 0)
    first_halos += start(send(("r", r, r)))
    r3 = start(send(("r3", r, r)))

    def keep_mass(y, h, g, total):
        cr[DEEP + y, h, pl.ds(COARSE_PAD + 8 * g, 8), :] = 0.8 / (4.0 + total)
    coarse_sums(sums, keep_mass)

    def region(src, dst, y0, y1, starts, load, rate):
        step = next(k for k in (8, 6, 4, 3, 2, 1) if (y1 - y0) % k == 0 and k * len(starts) <= 18)

        def body(i, carry):
            y = y0 + step * i
            for h in range(halves):
                for x in starts:
                    column = [at(src, y + j, h, x) for j in range(-1, step + 1)]
                    for j in range(step):
                        total = (column[j] + column[j + 2]) + (at(src, y + j, h, x - 1) + at(src, y + j, h, x + 1))
                        new = 0.2 * column[j + 1] + at(rate, y + j, h, x) * (at(load, y + j, h, x) + total)
                        dst[y + j, h, pl.ds(x, 8), :] = new
            return carry
        lax.fori_loop(0, (y1 - y0) // step, body, 0)

    def interior(src, dst, inset):
        region(src, dst, ROW_PAD + inset, ROW_PAD + ny - inset, windows(COL_PAD, nx, -inset), f, r)

    def frame(src, dst, inset, reach):
        full = windows(COL_PAD, nx, reach)
        region(src, dst, ROW_PAD - reach, ROW_PAD + inset, own, f, r)
        region(src, dst, ROW_PAD + ny - inset, ROW_PAD + ny + reach, own, f, r)
        region(src, dst, ROW_PAD, ROW_PAD + ny, [full[0], full[-1]], f, r)

    def defect(y0, y1, starts):
        def one(y):
            for h in range(halves):
                for x in starts:
                    a, b, c, e = left_over(ua, f, d, ROW_PAD + RATIO * y, h, x)
                    sums[y, h, pl.ds(x - COL_PAD, 8), :] = (a + b) + (c + e)
        loop(y0, y1, 2 if len(starts) <= 2 else 1, one)

    interior(ua, ub, 1)
    interior(ub, uc, 2)
    arrived(first_halos)
    frame(ua, ub, 1, 1)
    frame(ub, uc, 2, 0)
    u2 = start(send(("u2", uc, uc)))
    coarse_mass = start(send(("cr", cr, cr)))
    gone(first_halos)

    interior(uc, ua, 1)
    defect(1, cy - 1, own[1:-1])
    interior(ua, ud, 2)
    arrived(u2)
    frame(uc, ua, 1, 1)
    defect(0, 1, own)
    defect(cy - 1, cy, own)
    defect(1, cy - 1, [own[0], own[-1]])

    def keep_load(y, h, g, total):
        cl[DEEP + y, h, pl.ds(COARSE_PAD + 8 * g, 8), :] = total
    coarse_sums(sums, keep_load)
    coarse_load = start(send(("cl", cl, cl)))
    frame(ua, ud, 2, 0)
    v4 = start(send(("v4", ud, ud)))

    interior(ud, ub, 1)
    interior(ub, ue, 2)

    arrived(coarse_mass)
    arrived(coarse_load)

    def first_coarse(y):
        for h in range(halves):
            for x in windows(COARSE_PAD, cx, DEEP - 1):
                ca[y, h, pl.ds(x, 8), :] = at(cr, y, h, x) * at(cl, y, h, x)
    loop(1, cy + 2 * DEEP - 1, 4, first_coarse)

    order = [ca, cb, ca, cb, cc, ca, cb, ca, cb]
    for k in range(1, INNER):
        reach = FIRST - 1 - k if k < FIRST else INNER - k
        if k == FIRST:
            coarse_values = start(send(("cv", cc, cc)))
            arrived(v4)
            frame(ud, ub, 1, 1)
            frame(ub, ue, 2, 0)
            v6 = start(send(("v6", ue, ue)))
            arrived(coarse_values)
        region(order[k - 1], order[k], DEEP - reach, DEEP + cy + reach, windows(COARSE_PAD, cx, reach), cl, cr)
    now = order[-1]

    def spread_row(y):
        for h in range(halves):
            for w in range((cx + 2 + 7) // 8):
                c = at(now, DEEP - 1 + y, h, COARSE_PAD - 1 + 8 * w)
                for k in range(RATIO):
                    spread[y, h, pl.ds(32 * w + k, 8, stride=4), :] = c
    loop(0, cy + 2, 3, spread_row)

    arrived(r3)
    gone(u2)

    def swept(y, rows, starts):
        for h in range(halves):
            for x in starts:
                e = x - COL_PAD + 4
                here = spread[y, h, pl.ds(e, 8), :]
                beside = spread[y, h, pl.ds(e - 1, 8), :] + spread[y, h, pl.ds(e + 1, 8), :]
                kept = 0.2 * here
                for j in rows:
                    if j == 0:
                        total = beside + (here + spread[y - 1, h, pl.ds(e, 8), :])
                    elif j == RATIO - 1:
                        total = beside + (here + spread[y + 1, h, pl.ds(e, 8), :])
                    else:
                        total = beside + (here + here)
                    uc[RATIO * y + j, h, pl.ds(x, 8), :] = kept + at(r, RATIO * y + j, h, x) * total

    reach3 = windows(COL_PAD, nx, 3)

    def first_swept(y, carry):
        swept(y, range(RATIO), reach3)
        return carry
    lax.fori_loop(1, cy + 1, first_swept, 0)
    swept(0, range(1, RATIO), reach3)
    swept(cy + 1, range(RATIO - 1), reach3)

    starts = windows(COL_PAD, nx, 2)

    def second_swept(i, carry):
        for h in range(halves):
            for x in starts:
                swept_twice(uc, r, None, ub, ROW_PAD - 2 + 2 * i, h, x)
        return carry
    lax.fori_loop(0, (ny + 4) // 2, second_swept, 0)
    arrived(v6)

    for made in (r3, coarse_mass, coarse_load, v4, coarse_values, v6):
        gone(made)


def local(n_row, n_col, source_terms, initial_values, absorption):
    ny, nx, layers = source_terms.shape
    halves = layers // LANES
    sizes = (ny, nx, halves, n_row, n_col)
    _, _, count = plan(ny, nx)
    fine = (ny + 2 * ROW_PAD, halves, nx + 2 * COL_PAD, LANES)
    block = (ny, halves, nx, LANES)
    cy, cx = ny // RATIO, nx // RATIO
    coarse = pltpu.VMEM((cy + 2 * DEEP, halves, cx + 2 * COARSE_PAD, LANES), jnp.float32)

    def vmem(shape):
        return pltpu.VMEM(shape, jnp.float32)

    anywhere = pl.BlockSpec(memory_space=pltpu.HBM)
    inside = pl.BlockSpec(memory_space=pltpu.VMEM)
    held = pl.pallas_call(
        functools.partial(kernel, sizes),
        out_shape=(vmem(fine), vmem(fine), vmem(fine), vmem(block), vmem(fine)),
        in_specs=[anywhere] * 3,
        out_specs=(inside,) * 5,
        scratch_shapes=[
            vmem(fine), vmem(fine), vmem(fine),
            vmem((cy, halves, nx, LANES)),
            vmem((cy + 2, halves, (cx + 8) * RATIO, LANES)),
            coarse, coarse, coarse, coarse, coarse,
            pltpu.SemaphoreType.DMA((3 * halves,)),
            pltpu.SemaphoreType.DMA((count,)),
            pltpu.SemaphoreType.DMA((count,)),
        ],
        compiler_params=pltpu.CompilerParams(
            collective_id=0, has_side_effects=True, vmem_limit_bytes=25_300_000
        ),
        name="two_grids",
    )(source_terms, initial_values, absorption)
    shape = jax.ShapeDtypeStruct(source_terms.shape, jnp.float32)
    return pl.pallas_call(
        functools.partial(finish, (ny, nx, halves)),
        out_shape=(shape, shape),
        in_specs=[inside] * 5,
        out_specs=(anywhere, anywhere),
        scratch_shapes=[vmem(fine), vmem(block), pltpu.SemaphoreType.DMA((8 * halves,))],
        compiler_params=pltpu.CompilerParams(vmem_limit_bytes=14_000_000),
        name="finish",
    )(*held)


def solution(mesh):
    n_row, n_col = mesh.shape["row"], mesh.shape["col"]
    spec = P("row", "col", None)
    return jax.shard_map(
        functools.partial(local, n_row, n_col),
        mesh=mesh, in_specs=(spec, spec, spec), out_specs=(spec, spec), check_vma=False,
    )
```
